32 devices in a mesh: south: 2 (over x), east: 4 (over y, core), down: 4 (over z).
Axes of the slice: x: 2, y: 2, z: 4, core: 2. Of those that a mesh axis runs over, the one named last changes fastest.
Arguments:
- field_values: float32 [256, 32, 32, 128], P('south', 'east', 'down'), may hold values from 0.5 to 2
- flow_j: float32 [256, 32, 32, 128], P('south', 'east', 'down'), may hold values from -0.3 to 0.3
- flow_i: float32 [256, 32, 32, 128], P('south', 'east', 'down'), may hold values from -0.3 to 0.3
- flow_k: float32 [256, 32, 32, 128], P('south', 'east', 'down'), may hold values from -0.3 to 0.3
Outputs:
- standardized: float32 [256, 32, 32, 128], P('south', 'east', 'down')
- field_values_end: float32 [256, 32, 32, 128], P('south', 'east', 'down')
The draws below stay inside these ranges and needn't reach their ends.
All inputs are finite; a program needn't handle non-finite values.
Results may differ from the reference program's by a relative error of at most 0.00002.
Values sent between devices are 32-bit elements; how exact they have to be, the bound alone decides.
A program may use at most 128 MiB of HBM per device.

```python
import jax
import jax.numpy as jnp
from jax import lax

GRID_J = 256
GRID_I = 32
GRID_K = 32
LEVELS = 128
STEPS = 6


def block_scale(key, shape, cuts, smallest, high):
    def one(dim, blocks):
        steps = jax.random.uniform(jax.random.fold_in(jax.random.fold_in(key, 6), dim), (blocks,), jnp.float32, smallest / len(cuts), high / len(cuts))
        return jnp.repeat(jnp.exp(steps), shape[dim] // blocks).reshape((-1,) + (1,) * (len(shape) - dim - 1))

    level = one(*cuts[0])
    for cut in cuts[1:]:
        level = level * one(*cut)
    return level


def setup_inputs(seed: int = 0) -> dict:
    key_of = jax.random.split(jax.random.key(seed), 5)
    return {
        "field_values": jnp.clip(0.5 + 1.5 * jax.random.uniform(key_of[0], (GRID_J, GRID_I, GRID_K, LEVELS), jnp.float32) ** block_scale(key_of[0], (GRID_J, GRID_I, GRID_K, LEVELS), ((0, 2), (1, 4), (2, 4)), -0.2, 0.2), 0.5, 2.0),
        "flow_j": jnp.clip(jax.random.uniform(key_of[1], (GRID_J, GRID_I, GRID_K, LEVELS), jnp.float32, -0.3, 0.3) * block_scale(key_of[1], (GRID_J, GRID_I, GRID_K, LEVELS), ((0, 2), (1, 4), (2, 4)), -0.4, 0.0), -0.3, 0.3),
        "flow_i": jnp.clip(jax.random.uniform(key_of[2], (GRID_J, GRID_I, GRID_K, LEVELS), jnp.float32, -0.3, 0.3) * block_scale(key_of[2], (GRID_J, GRID_I, GRID_K, LEVELS), ((0, 2), (1, 4), (2, 4)), -0.4, 0.0), -0.3, 0.3),
        "flow_k": jnp.clip(jax.random.uniform(key_of[3], (GRID_J, GRID_I, GRID_K, LEVELS), jnp.float32, -0.3, 0.3) * block_scale(key_of[3], (GRID_J, GRID_I, GRID_K, LEVELS), ((0, 2), (1, 4), (2, 4)), -0.4, 0.0), -0.3, 0.3),
    }


def inner_cells(values, dims):
    for dim in dims:
        values = lax.slice_in_dim(values, 1, values.shape[dim] - 1, axis=dim)
    return values

def side_cells(values, dim, start, dims):
    others = [other for other in dims if other != dim]
    values = inner_cells(values, others)
    return lax.slice_in_dim(values, start, start + values.shape[dim] - 2, axis=dim)

def advance(padded, flow_j, flow_i, flow_k):
    middle = inner_cells(padded, (0, 1, 2))
    lower = [side_cells(padded, dim, 0, (0, 1, 2)) for dim in (0, 1, 2)]
    upper = [side_cells(padded, dim, 2, (0, 1, 2)) for dim in (0, 1, 2)]
    slopes = [above - below for above, below in zip(upper, lower)]
    smooth_rate = 0.05
    spread = lower[0] + upper[0] + lower[1] + upper[1] + lower[2] + upper[2] - 6.0 * middle
    return middle - flow_j * slopes[0] - flow_i * slopes[1] - flow_k * slopes[2] + smooth_rate * spread

def reference(field_values, flow_j, flow_i, flow_k):
    for step in range(STEPS):
        field_values = advance(jnp.pad(field_values, ((1, 1), (1, 1), (1, 1), (0, 0)), mode='constant'), flow_j, flow_i, flow_k)
    line_mean = lax.optimization_barrier(jnp.mean(field_values, axis=0, keepdims=True))
    centred = field_values - line_mean
    line_variance = lax.optimization_barrier(jnp.mean(centred * centred, axis=0, keepdims=True))
    standardized = centred * lax.rsqrt(line_variance + 0.0001)
    return (standardized, field_values)
```

```python
import functools

import jax
import jax.numpy as jnp
from jax import lax
from jax.experimental import pallas as pl
from jax.experimental.pallas import tpu as pltpu
from jax.sharding import PartitionSpec as P

STEPS = 6
CHUNKS = 2
BLOCK = 8
MESH = pl.DeviceIdType.MESH


def transport(counts, chunks, steps, field, flow_j, flow_i, flow_k, end, mean_out, scale_out,
              cells, flows, face_out, face_in, stats,
              load_sem, flow_sem, k_send, k_recv, i_send, i_recv, j_send, j_recv,
              stat_send, stat_recv):
    n_south, n_east, n_down = counts
    nj, ni, nk, _ = field.shape
    span = nj // chunks
    blocks = span // BLOCK
    south, east, down = (lax.axis_index(a) for a in ("south", "east", "down"))
    place = {"south": (south, n_south), "east": (east, n_east), "down": (down, n_down)}
    upward = lax.rem(east, 2) == 1

    def has(axis, side):
        me, count = place[axis]
        return me > 0 if side == 0 else me < count - 1

    def beside(axis, side):
        me, _ = place[axis]
        return {axis: me - 1 if side == 0 else me + 1}

    def row_of(turn):
        return jnp.where(upward, turn, ni - 1 - turn)

    def load(i, c):
        return pltpu.make_async_copy(
            field.at[pl.ds(c * span, span), i],
            cells.at[0, i + 1, pl.ds(c * span + 1, span)],
            load_sem.at[i, c],
        )

    def load_flow(d, i):
        source = (flow_j, flow_i, flow_k)[d]
        return pltpu.make_async_copy(source.at[pl.ds(0, nj), i], flows.at[d, i], flow_sem.at[d, i])

    def k_copy(slot, side, i, c):
        part = pl.ds(pl.multiple_of(c * span, BLOCK), span)
        return pltpu.make_async_remote_copy(
            face_out.at[slot, side, i, part], face_in.at[slot, 1 - side, i, part],
            k_send.at[slot, side, i, c], k_recv.at[slot, 1 - side, i, c],
            device_id=beside("down", side), device_id_type=MESH,
        )

    def i_copy(slot, side, c):
        part = pl.ds(c * span + 1, span)
        return pltpu.make_async_remote_copy(
            cells.at[slot, 1 if side == 0 else ni, part],
            cells.at[slot, ni + 1 if side == 0 else 0, part],
            i_send.at[slot, side, c], i_recv.at[slot, 1 - side, c],
            device_id=beside("east", side), device_id_type=MESH,
        )

    def j_copy(slot, side, i):
        return pltpu.make_async_remote_copy(
            cells.at[slot, i + 1, 1 if side == 0 else nj],
            cells.at[slot, i + 1, nj + 1 if side == 0 else 0],
            j_send.at[slot, side, i], j_recv.at[slot, 1 - side, i],
            device_id=beside("south", side), device_id_type=MESH,
        )

    def at_edge(axis, side, i, c):
        if axis == "east":
            return has(axis, side) & (i == (0 if side == 0 else ni - 1))
        return has(axis, side) & (c == (0 if side == 0 else chunks - 1))

    def each_copy(slot, i, c, act):
        for side in (0, 1):
            pl.when(has("down", side))(lambda: act(k_copy(slot, side, i, c)))
        for side in (0, 1):
            pl.when(at_edge("east", side, i, c))(lambda: act(i_copy(slot, side, c)))
        for side in (0, 1):
            pl.when(at_edge("south", side, i, c))(lambda: act(j_copy(slot, side, i)))

    def send(slot, i, c):
        each_copy(slot, i, c, lambda copy: copy.start())

    def sent(slot, i, c):
        each_copy(slot, i, c, lambda copy: copy.wait_send())

    def received(slot, i, c):
        for side in (0, 1):
            pl.when(has("down", side))(lambda: k_copy(slot, 1 - side, i, c).wait_recv())
        for side in (0, 1):
            pl.when(at_edge("east", side, i, c))(lambda: i_copy(slot, 1 - side, c).wait_recv())
        for side in (0, 1):
            pl.when(at_edge("south", side, i, c))(
                lambda: j_copy(slot, 1 - side, i).wait_recv()
            )

    barrier = pltpu.get_barrier_semaphore()
    for axis in ("east", "down"):
        for side in (0, 1):
            @pl.when(has(axis, side))
            def _():
                pl.semaphore_signal(barrier, 1, device_id=beside(axis, side), device_id_type=MESH)
    for offset in range(1, n_south):
        other = {"south": lax.rem(south + offset, n_south)}
        pl.semaphore_signal(barrier, 1, device_id=other, device_id_type=MESH)

    @pl.loop(0, ni * chunks)
    def _(unit):
        load(row_of(unit // chunks), unit % chunks).start()

    peers = n_south - 1
    for axis in ("east", "down"):
        for side in (0, 1):
            peers = peers + has(axis, side).astype(jnp.int32)
    pl.semaphore_wait(barrier, peers)

    @pl.loop(0, ni * chunks)
    def _(unit):
        i, c = row_of(unit // chunks), unit % chunks
        load(i, c).wait()

        @pl.loop(0, blocks)
        def _(block):
            j = pl.multiple_of(c * span + block * BLOCK, BLOCK)
            values = cells[0, i + 1, pl.ds(j + 1, BLOCK)]
            face_out[0, 0, i, pl.ds(j, BLOCK)] = values[:, 0, :]
            face_out[0, 1, i, pl.ds(j, BLOCK)] = values[:, nk - 1, :]

        send(0, i, c)

        @pl.when(c == chunks - 1)
        def _():
            for d in range(3):
                load_flow(d, i).start()

    for side in (0, 1):
        @pl.when(jnp.logical_not(has("down", side)))
        def _():
            @pl.loop(0, ni)
            def _(i):
                for slot in (0, 1):
                    face_in[slot, side, i] = jnp.zeros(face_in.shape[3:], jnp.float32)

        @pl.when(jnp.logical_not(has("east", side)))
        def _():
            @pl.loop(0, nj)
            def _(j):
                for slot in (0, 1):
                    cells[slot, 0 if side == 0 else ni + 1, j + 1] = jnp.zeros(
                        cells.shape[3:], jnp.float32)

        @pl.when(jnp.logical_not(has("south", side)))
        def _():
            @pl.loop(0, ni)
            def _(i):
                for slot in (0, 1):
                    cells[slot, i + 1, 0 if side == 0 else nj + 1] = jnp.zeros(
                        cells.shape[3:], jnp.float32)

    height = lax.broadcasted_iota(jnp.int32, (BLOCK,) + cells.shape[3:], 1)

    def advanced(slot, i, j):
        column = cells[slot, i + 1, pl.ds(j, BLOCK + 2)]
        j_low, middle, j_high = (column[s:s + BLOCK] for s in range(3))
        i_low = cells[slot, i, pl.ds(j + 1, BLOCK)]
        i_high = cells[slot, i + 2, pl.ds(j + 1, BLOCK)]
        k_low = jnp.where(
            height == 0, face_in[slot, 0, i, pl.ds(j, BLOCK)][:, None, :],
            pltpu.roll(middle, 1, 1))
        k_high = jnp.where(
            height == nk - 1, face_in[slot, 1, i, pl.ds(j, BLOCK)][:, None, :],
            pltpu.roll(middle, nk - 1, 1))
        spread = (j_low + j_high) + (i_low + i_high) + (k_low + k_high) - 6.0 * middle
        here = pl.ds(j, BLOCK)
        drift = (flows[0, i, here] * (j_high - j_low) + flows[1, i, here] * (i_high - i_low)
                 + flows[2, i, here] * (k_high - k_low))
        return middle - drift + 0.05 * spread

    @pl.loop(1, steps)
    def _(step):
        now, later = lax.rem(step + 1, 2), lax.rem(step, 2)

        @pl.loop(0, ni * chunks)
        def _(unit):
            i, c = row_of(unit // chunks), unit % chunks

            @pl.when((step == 1) & (c == 0))
            def _():
                for d in range(3):
                    load_flow(d, i).wait()

            @pl.when(step >= 2)
            def _():
                sent(later, i, c)

            received(now, i, c)

            @pl.loop(0, blocks)
            def _(block):
                j = pl.multiple_of(c * span + block * BLOCK, BLOCK)
                values = advanced(now, i, j)
                cells[later, i + 1, pl.ds(j + 1, BLOCK)] = values
                face_out[later, 0, i, pl.ds(j, BLOCK)] = values[:, 0, :]
                face_out[later, 1, i, pl.ds(j, BLOCK)] = values[:, nk - 1, :]

            send(later, i, c)

    now, later = (steps - 1) % 2, steps % 2
    zero = jnp.zeros(cells.shape[3:], jnp.float32)

    def stat_copy(offset, owner, i):
        target = lax.rem(south + offset, n_south)
        return pltpu.make_async_remote_copy(
            stats.at[owner, i], stats.at[owner, i],
            stat_send.at[offset - 1, i], stat_recv.at[offset - 1, i],
            device_id={"south": target}, device_id_type=MESH,
        )

    @pl.loop(0, ni)
    def _(turn):
        i = row_of(turn)

        def chunk(c, total):
            received(now, i, c)

            def block(b, total):
                j = pl.multiple_of(c * span + b * BLOCK, BLOCK)
                values = advanced(now, i, j)
                end[pl.ds(j, BLOCK), i] = values
                return total + jnp.sum(values, axis=0)

            return lax.fori_loop(0, blocks, block, total)

        own_mean = lax.fori_loop(0, chunks, chunk, zero) * (1.0 / nj)

        def square(b, total):
            centred = end[pl.ds(b * BLOCK, BLOCK), i] - own_mean
            return total + jnp.sum(centred * centred, axis=0)

        stats[south, i, 0] = own_mean
        stats[south, i, 1] = lax.fori_loop(0, nj // BLOCK, square, zero)
        for offset in range(1, n_south):
            stat_copy(offset, south, i).start()

    @pl.loop(0, ni * chunks)
    def _(unit):
        i, c = row_of(unit // chunks), unit % chunks
        sent(later, i, c)
        sent(now, i, c)

    @pl.loop(0, ni)
    def _(turn):
        i = row_of(turn)
        for offset in range(1, n_south):
            owner = lax.rem(south + n_south - offset, n_south)
            stat_copy(offset, owner, i).wait_recv()
        whole_mean = stats[0, i, 0]
        for other in range(1, n_south):
            whole_mean = whole_mean + stats[other, i, 0]
        whole_mean = whole_mean * (1.0 / n_south)
        whole_squares = zero
        for other in range(n_south):
            away = stats[other, i, 0] - whole_mean
            whole_squares = whole_squares + (stats[other, i, 1] + nj * (away * away))
        mean_out[i] = whole_mean
        scale_out[i] = lax.rsqrt(whole_squares * (1.0 / (nj * n_south)) + 0.0001)

    @pl.loop(0, ni)
    def _(i):
        for offset in range(1, n_south):
            stat_copy(offset, south, i).wait_send()


def scale(pieces, values, mean, factor, standardized, copied, scaled, copy_sem, scale_sem):
    rows = values.shape[0] // pieces

    def copy_out(c):
        part = pl.ds(c * rows, rows)
        return pltpu.make_async_copy(values.at[part], copied.at[part], copy_sem.at[c])

    def scale_out(c):
        part = pl.ds(c * rows, rows)
        return pltpu.make_async_copy(scaled.at[part], standardized.at[part], scale_sem.at[c])

    @pl.loop(0, pieces)
    def _(c):
        copy_out(c).start()

    @pl.loop(0, pieces)
    def _(c):
        @pl.loop(0, rows)
        def _(offset):
            r = c * rows + offset
            scaled[r] = (values[r] - mean[...]) * factor[...]

        scale_out(c).start()

    @pl.loop(0, pieces)
    def _(c):
        copy_out(c).wait()
        scale_out(c).wait()


def per_device(counts, field_values, flow_j, flow_i, flow_k):
    nj, ni, nk, levels = field_values.shape
    chunks = CHUNKS
    n_south = counts[0]
    plane = (ni, nk, levels)
    whole = jax.ShapeDtypeStruct(field_values.shape, jnp.float32)
    vmem = pl.BlockSpec(memory_space=pltpu.VMEM)
    hbm = pl.BlockSpec(memory_space=pltpu.HBM)
    dma = pltpu.SemaphoreType.DMA
    others = max(n_south - 1, 1)
    end, mean, factor = pl.pallas_call(
        functools.partial(transport, counts, chunks, STEPS),
        name="transport",
        out_shape=(
            whole,
            jax.ShapeDtypeStruct(plane, jnp.float32),
            jax.ShapeDtypeStruct(plane, jnp.float32),
        ),
        in_specs=[hbm] * 4,
        out_specs=(vmem,) * 3,
        scratch_shapes=[
            pltpu.VMEM((2, ni + 2, nj + 2, nk, levels), jnp.float32),
            pltpu.VMEM((3, ni, nj, nk, levels), jnp.float32),
            pltpu.VMEM((2, 2, ni, nj, levels), jnp.float32),
            pltpu.VMEM((2, 2, ni, nj, levels), jnp.float32),
            pltpu.VMEM((n_south, ni, 2, nk, levels), jnp.float32),
            dma((ni, chunks)),
            dma((3, ni)),
            dma((2, 2, ni, chunks)),
            dma((2, 2, ni, chunks)),
            dma((2, 2, chunks)),
            dma((2, 2, chunks)),
            dma((2, 2, ni)),
            dma((2, 2, ni)),
            dma((others, ni)),
            dma((others, ni)),
        ],
        compiler_params=pltpu.CompilerParams(
            collective_id=0, has_side_effects=True, vmem_limit_bytes=40 * 2**20
        ),
    )(*(pltpu.with_memory_space_constraint(array, pltpu.HBM)
        for array in (field_values, flow_j, flow_i, flow_k)))
    pieces = 8
    return pl.pallas_call(
        functools.partial(scale, pieces),
        name="scale",
        in_specs=[vmem] * 3,
        out_specs=(hbm, hbm),
        out_shape=(whole, whole),
        scratch_shapes=[
            pltpu.VMEM(field_values.shape, jnp.float32),
            dma((pieces,)),
            dma((pieces,)),
        ],
        compiler_params=pltpu.CompilerParams(vmem_limit_bytes=16 * 2**20),
    )(end, mean, factor)


def solution(mesh):
    counts = tuple(mesh.shape[axis] for axis in ("south", "east", "down"))
    spec = P("south", "east", "down", None)
    return jax.shard_map(
        functools.partial(per_device, counts),
        mesh=mesh,
        in_specs=(spec,) * 4,
        out_specs=(spec, spec),
        check_vma=False,
    )
```

```python
import functools

import jax
import jax.numpy as jnp
from jax import lax
from jax.experimental import pallas as pl
from jax.experimental.pallas import tpu as pltpu
from jax.sharding import PartitionSpec as P

STEPS = 6
BLOCK = 8
MESH = pl.DeviceIdType.MESH


def transport(counts, steps, field, flow_j, flow_i, flow_k, end, mean_out, scale_out,
              cells, flows, face_out, face_in, stats,
              ready_down, ready_east, ready_south, load_sem, flow_sem,
              k_send, k_recv, i_send, i_recv, j_send, j_recv, stat_send, stat_recv):
    n_south, n_east, n_down = counts
    nj, ni, nk, _ = field.shape
    blocks = nj // BLOCK
    half = ni // 2
    early = ni - 2
    south, east, down = (lax.axis_index(a) for a in ("south", "east", "down"))
    place = {"south": (south, n_south), "east": (east, n_east), "down": (down, n_down)}
    upward = lax.rem(east, 2) == 1

    def has(axis, side):
        me, count = place[axis]
        return me > 0 if side == 0 else me < count - 1

    def beside(axis, side):
        me, _ = place[axis]
        return {axis: me - 1 if side == 0 else me + 1}

    def row_of(turn):
        return jnp.where(upward, turn, ni - 1 - turn)

    def rows_of(first, count):
        return pl.ds(jnp.where(upward, first, ni - first - count), count)

    def load(turn):
        i = row_of(turn)
        return pltpu.make_async_copy(
            field.at[pl.ds(0, nj), i], cells.at[0, i + 1, pl.ds(1, nj)],
            load_sem.at[jnp.minimum(turn, 2)],
        )

    def loaded(first, count):
        start = jnp.where(upward, first, ni - first - count)
        part = cells.at[0, pl.ds(start + 1, count), pl.ds(1, nj)]
        pltpu.make_async_copy(part, part, load_sem.at[first]).wait()

    def load_flows(turn):
        i = row_of(turn)
        for d, source in enumerate((flow_j, flow_i, flow_k)):
            pltpu.make_async_copy(
                source.at[pl.ds(0, nj), i], flows.at[d, i], flow_sem.at[jnp.where(turn < 2, 0, 1)]
            ).start()

    def flows_loaded(group):
        rows = rows_of(0, 2) if group == 0 else rows_of(2, early)
        part = flows.at[pl.ds(0, 3), rows]
        pltpu.make_async_copy(part, part, flow_sem.at[group]).wait()

    def k_copy(slot, side, i):
        return pltpu.make_async_remote_copy(
            face_out.at[slot, side, i], face_in.at[slot, 1 - side, i],
            k_send.at[i], k_recv.at[slot, i],
            device_id=beside("down", side), device_id_type=MESH,
        )

    def k_both(slot, i):
        return pltpu.make_async_remote_copy(
            face_out.at[slot, pl.ds(0, 2), i], face_in.at[slot, pl.ds(0, 2), i],
            k_send.at[i], k_recv.at[slot, i],
            device_id=beside("down", 0), device_id_type=MESH,
        )

    def i_copy(slot, side):
        part = pl.ds(1, nj)
        return pltpu.make_async_remote_copy(
            cells.at[slot, 1 if side == 0 else ni, part],
            cells.at[slot, ni + 1 if side == 0 else 0, part],
            i_send.at[side], i_recv.at[slot, 1 - side],
            device_id=beside("east", side), device_id_type=MESH,
        )

    def j_copy(slot, side, group):
        rows = pl.ds(jnp.where(upward, group * half, ni - (group + 1) * half) + 1, half)
        sending, receiving = (side, 1 - side) if n_south > 2 else (0, 0)
        return pltpu.make_async_remote_copy(
            cells.at[slot, rows, 1 if side == 0 else nj],
            cells.at[slot, rows, nj + 1 if side == 0 else 0],
            j_send.at[sending, group], j_recv.at[slot, receiving, group],
            device_id=beside("south", side), device_id_type=MESH,
        )

    def edge_turn(side):
        return jnp.where(upward == (side == 0), 0, ni - 1)

    def each_k(act):
        if n_down > 1:
            inside = has("down", 0) & has("down", 1)
            pl.when(inside)(lambda: act(k_both))
            pl.when(jnp.logical_not(inside))(lambda: act(lambda slot, i: k_copy(slot, 0, i)))

    def sent(slot, turn):
        each_k(lambda copy: copy(slot, row_of(turn)).wait_send())

    def received(slot, turn):
        each_k(lambda copy: copy(slot, row_of(turn)).wait_recv())
        for side in (0, 1):
            pl.when(has("east", side) & (turn == edge_turn(side)))(
                lambda: i_copy(slot, 1 - side).wait_recv())
        for group in (0, 1):
            for side in (0, 1):
                pl.when(has("south", side) & (turn == group * half))(
                    lambda: j_copy(slot, 1 - side, group).wait_recv())

    def send_k(slot, side, turn):
        pl.when(has("down", side))(lambda: k_copy(slot, side, row_of(turn)).start())

    def send(slot, turn):
        for side in (0, 1):
            send_k(slot, side, turn)
        for side in (0, 1):
            @pl.when(has("east", side) & (turn == edge_turn(side)))
            def _():
                i_copy(slot, side).wait_send()
                i_copy(slot, side).start()
        for group in (0, 1):
            for side in (0, 1):
                @pl.when(has("south", side) & (turn == (group + 1) * half - 1))
                def _():
                    j_copy(slot, side, group).wait_send()
                    j_copy(slot, side, group).start()

    barrier = pltpu.get_barrier_semaphore()
    lower = south
    for offset in range(1, n_south):
        @pl.when(south + offset < n_south)
        def _():
            pl.semaphore_signal(barrier, 1, device_id={"south": south + offset},
                                device_id_type=MESH)
    for axis in ("down", "east"):
        lower = lower + has(axis, 0).astype(jnp.int32)

        @pl.when(has(axis, 1))
        def _():
            pl.semaphore_signal(barrier, 1, device_id=beside(axis, 1), device_id_type=MESH)

    @pl.loop(0, ni)
    def _(turn):
        load(turn).start()

    pl.when(lower > 0)(lambda: pl.semaphore_wait(barrier, lower))
    for axis, ready in (("down", ready_down), ("east", ready_east)):
        @pl.when(has(axis, 0))
        def _():
            pl.semaphore_signal(ready, 1, device_id=beside(axis, 0), device_id_type=MESH)
    for offset in range(1, n_south):
        @pl.when(south - offset >= 0)
        def _():
            pl.semaphore_signal(ready_south, 1, device_id={"south": south - offset},
                                device_id_type=MESH)

    def extract(turn):
        i = row_of(turn)

        @pl.loop(0, blocks)
        def _(block):
            j = pl.multiple_of(block * BLOCK, BLOCK)
            values = cells[0, i + 1, pl.ds(j + 1, BLOCK)]
            face_out[0, 0, i, pl.ds(j, BLOCK)] = values[:, 0, :]
            face_out[0, 1, i, pl.ds(j, BLOCK)] = values[:, nk - 1, :]

    for turn in (0, 1):
        loaded(turn, 1)
        extract(turn)
        send_k(0, 0, turn)
    pl.when(has("down", 1))(lambda: pl.semaphore_wait(ready_down, 1))
    for turn in (0, 1):
        send_k(0, 1, turn)
    loaded(2, early)

    @pl.loop(2, ni)
    def _(turn):
        extract(turn)
        for side in (0, 1):
            send_k(0, side, turn)

    @pl.loop(0, ni)
    def _(turn):
        load_flows(turn)

    pl.when(has("east", 1))(lambda: pl.semaphore_wait(ready_east, 1))
    for side in (0, 1):
        pl.when(has("east", side))(lambda: i_copy(0, side).start())
    if n_south > 1:
        pl.when(has("south", 1))(lambda: pl.semaphore_wait(ready_south, n_south - 1 - south))
    for group in (0, 1):
        for side in (0, 1):
            pl.when(has("south", side))(lambda: j_copy(0, side, group).start())

    for side in (0, 1):
        @pl.when(jnp.logical_not(has("down", side)))
        def _():
            @pl.loop(0, ni)
            def _(i):
                for slot in (0, 1):
                    face_in[slot, side, i] = jnp.zeros(face_in.shape[3:], jnp.float32)

        @pl.when(jnp.logical_not(has("east", side)))
        def _():
            @pl.loop(0, nj)
            def _(j):
                for slot in (0, 1):
                    cells[slot, 0 if side == 0 else ni + 1, j + 1] = jnp.zeros(
                        cells.shape[3:], jnp.float32)

        @pl.when(jnp.logical_not(has("south", side)))
        def _():
            @pl.loop(0, ni)
            def _(i):
                for slot in (0, 1):
                    cells[slot, i + 1, 0 if side == 0 else nj + 1] = jnp.zeros(
                        cells.shape[3:], jnp.float32)

    height = lax.broadcasted_iota(jnp.int32, (BLOCK,) + cells.shape[3:], 1)

    def advanced(slot, i, j):
        column = cells[slot, i + 1, pl.ds(j, BLOCK + 2)]
        j_low, middle, j_high = (column[s:s + BLOCK] for s in range(3))
        i_low = cells[slot, i, pl.ds(j + 1, BLOCK)]
        i_high = cells[slot, i + 2, pl.ds(j + 1, BLOCK)]
        k_low = jnp.where(
            height == 0, face_in[slot, 0, i, pl.ds(j, BLOCK)][:, None, :],
            pltpu.roll(middle, 1, 1))
        k_high = jnp.where(
            height == nk - 1, face_in[slot, 1, i, pl.ds(j, BLOCK)][:, None, :],
            pltpu.roll(middle, nk - 1, 1))
        spread = (j_low + j_high) + (i_low + i_high) + (k_low + k_high) - 6.0 * middle
        here = pl.ds(j, BLOCK)
        drift = (flows[0, i, here] * (j_high - j_low) + flows[1, i, here] * (i_high - i_low)
                 + flows[2, i, here] * (k_high - k_low))
        return middle - drift + 0.05 * spread

    @pl.loop(1, steps)
    def _(step):
        now, later = lax.rem(step + 1, 2), lax.rem(step, 2)

        @pl.loop(0, ni)
        def _(turn):
            i = row_of(turn)
            for group, first in enumerate((0, 2)):
                pl.when((step == 1) & (turn == first))(lambda: flows_loaded(group))
            sent(now, turn)
            received(now, turn)

            @pl.loop(0, blocks)
            def _(block):
                j = pl.multiple_of(block * BLOCK, BLOCK)
                values = advanced(now, i, j)
                cells[later, i + 1, pl.ds(j + 1, BLOCK)] = values
                face_out[later, 0, i, pl.ds(j, BLOCK)] = values[:, 0, :]
                face_out[later, 1, i, pl.ds(j, BLOCK)] = values[:, nk - 1, :]

            send(later, turn)

    now = (steps - 1) % 2
    zero = jnp.zeros(cells.shape[3:], jnp.float32)

    def stat_copy(offset, owner, part):
        target = lax.rem(south + offset, n_south)
        rows = rows_of(0, early) if part == 0 else rows_of(early, 2)
        return pltpu.make_async_remote_copy(
            stats.at[owner, rows], stats.at[owner, rows],
            stat_send.at[offset - 1, part], stat_recv.at[offset - 1, part],
            device_id={"south": target}, device_id_type=MESH,
        )

    @pl.loop(0, ni)
    def _(turn):
        i = row_of(turn)
        received(now, turn)

        def block(b, total):
            j = pl.multiple_of(b * BLOCK, BLOCK)
            values = advanced(now, i, j)
            end[pl.ds(j, BLOCK), i] = values
            return total + jnp.sum(values, axis=0)

        own_mean = lax.fori_loop(0, blocks, block, zero) * (1.0 / nj)

        def square(b, total):
            centred = end[pl.ds(b * BLOCK, BLOCK), i] - own_mean
            return total + jnp.sum(centred * centred, axis=0)

        stats[south, i, 0] = own_mean
        stats[south, i, 1] = lax.fori_loop(0, blocks, square, zero)
        for part, last in enumerate((early - 1, ni - 1)):
            @pl.when(turn == last)
            def _():
                for offset in range(1, n_south):
                    stat_copy(offset, south, part).start()

    @pl.loop(0, ni)
    def _(turn):
        sent(now, turn)

    for side in (0, 1):
        pl.when(has("east", side))(lambda: i_copy(now, side).wait_send())
        for group in (0, 1):
            pl.when(has("south", side))(lambda: j_copy(now, side, group).wait_send())

    for part, (first, count) in enumerate(((0, early), (early, 2))):
        for offset in range(1, n_south):
            owner = lax.rem(south + n_south - offset, n_south)
            stat_copy(offset, owner, part).wait_recv()

        @pl.loop(first, first + count)
        def _(turn):
            i = row_of(turn)
            whole_mean = stats[0, i, 0]
            for other in range(1, n_south):
                whole_mean = whole_mean + stats[other, i, 0]
            whole_mean = whole_mean * (1.0 / n_south)
            whole_squares = zero
            for other in range(n_south):
                away = stats[other, i, 0] - whole_mean
                whole_squares = whole_squares + (stats[other, i, 1] + nj * (away * away))
            mean_out[i] = whole_mean
            scale_out[i] = lax.rsqrt(whole_squares * (1.0 / (nj * n_south)) + 0.0001)

    for part in (0, 1):
        for offset in range(1, n_south):
            stat_copy(offset, south, part).wait_send()


def scale(pieces, values, mean, factor, standardized, copied, scaled, copy_sem, scale_sem):
    rows = values.shape[0] // pieces

    def copy_out(c):
        part = pl.ds(c * rows, rows)
        return pltpu.make_async_copy(values.at[part], copied.at[part], copy_sem.at[c])

    def scale_out(c):
        part = pl.ds(c * rows, rows)
        return pltpu.make_async_copy(scaled.at[part], standardized.at[part], scale_sem.at[c])

    @pl.loop(0, pieces)
    def _(c):
        copy_out(c).start()

    @pl.loop(0, pieces)
    def _(c):
        @pl.loop(0, rows)
        def _(offset):
            r = c * rows + offset
            scaled[r] = (values[r] - mean[...]) * factor[...]

        scale_out(c).start()

    @pl.loop(0, pieces)
    def _(c):
        copy_out(c).wait()
        scale_out(c).wait()


def per_device(counts, field_values, flow_j, flow_i, flow_k):
    nj, ni, nk, levels = field_values.shape
    n_south = counts[0]
    plane = (ni, nk, levels)
    whole = jax.ShapeDtypeStruct(field_values.shape, jnp.float32)
    vmem = pl.BlockSpec(memory_space=pltpu.VMEM)
    hbm = pl.BlockSpec(memory_space=pltpu.HBM)
    dma = pltpu.SemaphoreType.DMA
    regular = pltpu.SemaphoreType.REGULAR
    others = max(n_south - 1, 1)
    sides = 2 if n_south > 2 else 1
    end, mean, factor = pl.pallas_call(
        functools.partial(transport, counts, STEPS),
        name="transport",
        out_shape=(
            whole,
            jax.ShapeDtypeStruct(plane, jnp.float32),
            jax.ShapeDtypeStruct(plane, jnp.float32),
        ),
        in_specs=[hbm] * 4,
        out_specs=(vmem,) * 3,
        scratch_shapes=[
            pltpu.VMEM((2, ni + 2, nj + 2, nk, levels), jnp.float32),
            pltpu.VMEM((3, ni, nj, nk, levels), jnp.float32),
            pltpu.VMEM((2, 2, ni, nj, levels), jnp.float32),
            pltpu.VMEM((2, 2, ni, nj, levels), jnp.float32),
            pltpu.VMEM((n_south, ni, 2, nk, levels), jnp.float32),
            regular,
            regular,
            regular,
            dma((3,)),
            dma((2,)),
            dma((ni,)),
            dma((2, ni)),
            dma((2,)),
            dma((2, 2)),
            dma((sides, 2)),
            dma((2, sides, 2)),
            dma((others, 2)),
            dma((others, 2)),
        ],
        compiler_params=pltpu.CompilerParams(
            collective_id=0, has_side_effects=True, vmem_limit_bytes=40 * 2**20
        ),
    )(*(pltpu.with_memory_space_constraint(array, pltpu.HBM)
        for array in (field_values, flow_j, flow_i, flow_k)))
    pieces = 8
    return pl.pallas_call(
        functools.partial(scale, pieces),
        name="scale",
        in_specs=[vmem] * 3,
        out_specs=(hbm, hbm),
        out_shape=(whole, whole),
        scratch_shapes=[
            pltpu.VMEM(field_values.shape, jnp.float32),
            dma((pieces,)),
            dma((pieces,)),
        ],
        compiler_params=pltpu.CompilerParams(vmem_limit_bytes=16 * 2**20),
    )(end, mean, factor)


def solution(mesh):
    counts = tuple(mesh.shape[axis] for axis in ("south", "east", "down"))
    spec = P("south", "east", "down", None)
    return jax.shard_map(
        functools.partial(per_device, counts),
        mesh=mesh,
        in_specs=(spec,) * 4,
        out_specs=(spec, spec),
        check_vma=False,
    )
```

```python
import functools

import jax
import jax.numpy as jnp
from jax import lax
from jax.experimental import pallas as pl
from jax.experimental.pallas import tpu as pltpu
from jax.sharding import PartitionSpec as P

STEPS = 6
BLOCK = 8
LEVEL = 4
MESH = pl.DeviceIdType.MESH


def transport(counts, steps, field, flow_j, flow_i, flow_k, end, mean_out, scale_out,
              cells, flows, stats,
              ready_down, ready_east, ready_south, load_sem, flow_sem,
              k_send, k_recv, i_send, i_recv, j_send, j_recv, stat_send, stat_recv):
    n_south, n_east, n_down = counts
    nj, ni, nk, levels = field.shape
    inner = pl.ds(LEVEL, nk)
    blocks = nj // BLOCK
    half = ni // 2
    early = ni - 2
    south, east, down = (lax.axis_index(a) for a in ("south", "east", "down"))
    place = {"south": (south, n_south), "east": (east, n_east), "down": (down, n_down)}
    upward = lax.rem(east, 2) == 1

    def has(axis, side):
        me, count = place[axis]
        return me > 0 if side == 0 else me < count - 1

    def beside(axis, side):
        me, _ = place[axis]
        return {axis: me - 1 if side == 0 else me + 1}

    def row_of(turn):
        return jnp.where(upward, turn, ni - 1 - turn)

    def rows_of(first, count):
        return pl.ds(jnp.where(upward, first, ni - first - count), count)

    def load(turn):
        i = row_of(turn)
        return pltpu.make_async_copy(
            field.at[pl.ds(0, nj), i], cells.at[0, i + 1, pl.ds(1, nj), inner],
            load_sem.at[jnp.minimum(turn, 2)],
        )

    def loaded(first, count):
        start = jnp.where(upward, first, ni - first - count)
        part = cells.at[0, pl.ds(start + 1, count), pl.ds(1, nj), inner]
        pltpu.make_async_copy(part, part, load_sem.at[first]).wait()

    def load_flows(turn):
        i = row_of(turn)
        for d, source in enumerate((flow_j, flow_i, flow_k)):
            pltpu.make_async_copy(
                source.at[pl.ds(0, nj), i], flows.at[d, i], flow_sem.at[jnp.where(turn < 2, 0, 1)]
            ).start()

    def flows_loaded(group):
        rows = rows_of(0, 2) if group == 0 else rows_of(2, early)
        part = flows.at[pl.ds(0, 3), rows]
        pltpu.make_async_copy(part, part, flow_sem.at[group]).wait()

    def edge(side):
        return LEVEL if side == 0 else LEVEL + nk - 1

    def halo(side):
        return LEVEL - 1 if side == 0 else LEVEL + nk

    def k_copy(slot, side, i):
        part = pl.ds(1, nj)
        return pltpu.make_async_remote_copy(
            cells.at[slot, i + 1, part, edge(side)], cells.at[slot, i + 1, part, halo(1 - side)],
            k_send.at[i], k_recv.at[slot, i],
            device_id=beside("down", side), device_id_type=MESH,
        )

    def k_both(slot, i):
        part = cells.at[slot, i + 1, pl.ds(1, nj), pl.ds(LEVEL, 2)]
        return pltpu.make_async_remote_copy(
            part, part, k_send.at[i], k_recv.at[slot, i],
            device_id=beside("down", 0), device_id_type=MESH,
        )

    def i_copy(slot, side):
        part = pl.ds(1, nj)
        return pltpu.make_async_remote_copy(
            cells.at[slot, 1 if side == 0 else ni, part, inner],
            cells.at[slot, ni + 1 if side == 0 else 0, part, inner],
            i_send.at[side], i_recv.at[slot, 1 - side],
            device_id=beside("east", side), device_id_type=MESH,
        )

    def j_copy(slot, side, group):
        rows = pl.ds(jnp.where(upward, group * half, ni - (group + 1) * half) + 1, half)
        sending, receiving = (side, 1 - side) if n_south > 2 else (0, 0)
        return pltpu.make_async_remote_copy(
            cells.at[slot, rows, 1 if side == 0 else nj, inner],
            cells.at[slot, rows, nj + 1 if side == 0 else 0, inner],
            j_send.at[sending, group], j_recv.at[slot, receiving, group],
            device_id=beside("south", side), device_id_type=MESH,
        )

    def edge_turn(side):
        return jnp.where(upward == (side == 0), 0, ni - 1)

    def each_k(act):
        if n_down > 1:
            inside = has("down", 0) & has("down", 1)
            pl.when(inside)(lambda: act(k_both))
            pl.when(jnp.logical_not(inside))(lambda: act(lambda slot, i: k_copy(slot, 0, i)))

    def sent(slot, turn):
        each_k(lambda copy: copy(slot, row_of(turn)).wait_send())

    def received(slot, turn):
        each_k(lambda copy: copy(slot, row_of(turn)).wait_recv())
        for side in (0, 1):
            pl.when(has("east", side) & (turn == edge_turn(side)))(
                lambda: i_copy(slot, 1 - side).wait_recv())
        for group in (0, 1):
            for side in (0, 1):
                pl.when(has("south", side) & (turn == group * half))(
                    lambda: j_copy(slot, 1 - side, group).wait_recv())

    def send_k(slot, side, turn):
        pl.when(has("down", side))(lambda: k_copy(slot, side, row_of(turn)).start())

    def send(slot, turn):
        for side in (0, 1):
            send_k(slot, side, turn)
        for side in (0, 1):
            @pl.when(has("east", side) & (turn == edge_turn(side)))
            def _():
                i_copy(slot, side).wait_send()
                i_copy(slot, side).start()
        for group in (0, 1):
            for side in (0, 1):
                @pl.when(has("south", side) & (turn == (group + 1) * half - 1))
                def _():
                    j_copy(slot, side, group).wait_send()
                    j_copy(slot, side, group).start()

    zero = jnp.zeros((nk, levels), jnp.float32)

    barrier = pltpu.get_barrier_semaphore()
    lower = south
    for offset in range(1, n_south):
        @pl.when(south + offset < n_south)
        def _():
            pl.semaphore_signal(barrier, 1, device_id={"south": south + offset},
                                device_id_type=MESH)
    for axis in ("down", "east"):
        lower = lower + has(axis, 0).astype(jnp.int32)

        @pl.when(has(axis, 1))
        def _():
            pl.semaphore_signal(barrier, 1, device_id=beside(axis, 1), device_id_type=MESH)

    @pl.loop(0, ni)
    def _(turn):
        load(turn).start()

    pl.when(lower > 0)(lambda: pl.semaphore_wait(barrier, lower))
    for axis, ready in (("down", ready_down), ("east", ready_east)):
        @pl.when(has(axis, 0))
        def _():
            pl.semaphore_signal(ready, 1, device_id=beside(axis, 0), device_id_type=MESH)
    for offset in range(1, n_south):
        @pl.when(south - offset >= 0)
        def _():
            pl.semaphore_signal(ready_south, 1, device_id={"south": south - offset},
                                device_id_type=MESH)

    for turn in (0, 1):
        loaded(turn, 1)
        send_k(0, 0, turn)
    pl.when(has("down", 1))(lambda: pl.semaphore_wait(ready_down, 1))
    for turn in (0, 1):
        send_k(0, 1, turn)
    loaded(2, early)

    @pl.loop(2, ni)
    def _(turn):
        for side in (0, 1):
            send_k(0, side, turn)

    @pl.loop(0, ni)
    def _(turn):
        load_flows(turn)

    pl.when(has("east", 1))(lambda: pl.semaphore_wait(ready_east, 1))
    for side in (0, 1):
        pl.when(has("east", side))(lambda: i_copy(0, side).start())
    if n_south > 1:
        pl.when(has("south", 1))(lambda: pl.semaphore_wait(ready_south, n_south - 1 - south))
    for group in (0, 1):
        for side in (0, 1):
            pl.when(has("south", side))(lambda: j_copy(0, side, group).start())

    for side in (0, 1):
        @pl.when(jnp.logical_not(has("down", side)))
        def _():
            @pl.loop(0, ni)
            def _(i):
                @pl.loop(0, blocks)
                def _(block):
                    for slot in (0, 1):
                        cells[slot, i + 1, pl.ds(block * BLOCK + 1, BLOCK), halo(side)] = (
                            jnp.zeros((BLOCK, levels), jnp.float32))

        @pl.when(jnp.logical_not(has("east", side)))
        def _():
            @pl.loop(0, nj)
            def _(j):
                for slot in (0, 1):
                    cells[slot, 0 if side == 0 else ni + 1, j + 1, inner] = zero

        @pl.when(jnp.logical_not(has("south", side)))
        def _():
            @pl.loop(0, ni)
            def _(i):
                for slot in (0, 1):
                    cells[slot, i + 1, 0 if side == 0 else nj + 1, inner] = zero

    def advanced(slot, i, j):
        here = pl.ds(j + 1, BLOCK)
        column = cells[slot, i + 1, pl.ds(j, BLOCK + 2), inner]
        middle = column[1:BLOCK + 1]
        sides = (
            (column[:BLOCK], column[2:]),
            (cells[slot, i, here, inner], cells[slot, i + 2, here, inner]),
            (cells[slot, i + 1, here, pl.ds(LEVEL - 1, nk)],
             cells[slot, i + 1, here, pl.ds(LEVEL + 1, nk)]),
        )
        around, drift = None, None
        for d, (low, high) in enumerate(sides):
            both = low + high
            moved = flows[d, i, pl.ds(j, BLOCK)] * (low - high)
            around = both if d == 0 else around + both
            drift = moved if d == 0 else drift + moved
        return (0.7 * middle + 0.05 * around) + drift

    @pl.loop(1, steps)
    def _(step):
        now, later = lax.rem(step + 1, 2), lax.rem(step, 2)

        @pl.loop(0, ni)
        def _(turn):
            i = row_of(turn)
            for group, first in enumerate((0, 2)):
                pl.when((step == 1) & (turn == first))(lambda: flows_loaded(group))
            sent(now, turn)
            received(now, turn)

            @pl.loop(0, blocks)
            def _(block):
                j = pl.multiple_of(block * BLOCK, BLOCK)
                values = advanced(now, i, j)
                cells[later, i + 1, pl.ds(j + 1, BLOCK), inner] = values

            send(later, turn)

    now = (steps - 1) % 2

    def stat_copy(offset, owner, part):
        target = lax.rem(south + offset, n_south)
        rows = rows_of(0, early) if part == 0 else rows_of(early, 2)
        return pltpu.make_async_remote_copy(
            stats.at[owner, rows], stats.at[owner, rows],
            stat_send.at[offset - 1, part], stat_recv.at[offset - 1, part],
            device_id={"south": target}, device_id_type=MESH,
        )

    @pl.loop(0, ni)
    def _(turn):
        i = row_of(turn)
        received(now, turn)

        def block(b, total):
            j = pl.multiple_of(b * BLOCK, BLOCK)
            values = advanced(now, i, j)
            end[pl.ds(j, BLOCK), i] = values
            return total + jnp.sum(values, axis=0)

        own_mean = lax.fori_loop(0, blocks, block, zero) * (1.0 / nj)

        def square(b, total):
            centred = end[pl.ds(b * BLOCK, BLOCK), i] - own_mean
            return total + jnp.sum(centred * centred, axis=0)

        stats[south, i, 0] = own_mean
        stats[south, i, 1] = lax.fori_loop(0, blocks, square, zero)
        for part, last in enumerate((early - 1, ni - 1)):
            @pl.when(turn == last)
            def _():
                for offset in range(1, n_south):
                    stat_copy(offset, south, part).start()

    @pl.loop(0, ni)
    def _(turn):
        sent(now, turn)

    for side in (0, 1):
        pl.when(has("east", side))(lambda: i_copy(now, side).wait_send())
        for group in (0, 1):
            pl.when(has("south", side))(lambda: j_copy(now, side, group).wait_send())

    for part, (first, count) in enumerate(((0, early), (early, 2))):
        for offset in range(1, n_south):
            owner = lax.rem(south + n_south - offset, n_south)
            stat_copy(offset, owner, part).wait_recv()

        @pl.loop(first, first + count)
        def _(turn):
            i = row_of(turn)
            whole_mean = stats[0, i, 0]
            for other in range(1, n_south):
                whole_mean = whole_mean + stats[other, i, 0]
            whole_mean = whole_mean * (1.0 / n_south)
            whole_squares = zero
            for other in range(n_south):
                away = stats[other, i, 0] - whole_mean
                whole_squares = whole_squares + (stats[other, i, 1] + nj * (away * away))
            mean_out[i] = whole_mean
            scale_out[i] = lax.rsqrt(whole_squares * (1.0 / (nj * n_south)) + 0.0001)

    for part in (0, 1):
        for offset in range(1, n_south):
            stat_copy(offset, south, part).wait_send()


def scale(pieces, values, mean, factor, standardized, copied, scaled, copy_sem, scale_sem):
    rows = values.shape[0] // pieces

    def copy_out(c):
        part = pl.ds(c * rows, rows)
        return pltpu.make_async_copy(values.at[part], copied.at[part], copy_sem.at[c])

    def scale_out(c):
        part = pl.ds(c * rows, rows)
        return pltpu.make_async_copy(scaled.at[part], standardized.at[part], scale_sem.at[c])

    @pl.loop(0, pieces)
    def _(c):
        copy_out(c).start()

    @pl.loop(0, pieces)
    def _(c):
        @pl.loop(0, rows)
        def _(offset):
            r = c * rows + offset
            scaled[r] = (values[r] - mean[...]) * factor[...]

        scale_out(c).start()

    @pl.loop(0, pieces)
    def _(c):
        copy_out(c).wait()
        scale_out(c).wait()


def per_device(counts, field_values, flow_j, flow_i, flow_k):
    nj, ni, nk, levels = field_values.shape
    n_south = counts[0]
    plane = (ni, nk, levels)
    whole = jax.ShapeDtypeStruct(field_values.shape, jnp.float32)
    vmem = pl.BlockSpec(memory_space=pltpu.VMEM)
    hbm = pl.BlockSpec(memory_space=pltpu.HBM)
    dma = pltpu.SemaphoreType.DMA
    regular = pltpu.SemaphoreType.REGULAR
    others = max(n_south - 1, 1)
    sides = 2 if n_south > 2 else 1
    end, mean, factor = pl.pallas_call(
        functools.partial(transport, counts, STEPS),
        name="transport",
        out_shape=(
            whole,
            jax.ShapeDtypeStruct(plane, jnp.float32),
            jax.ShapeDtypeStruct(plane, jnp.float32),
        ),
        in_specs=[hbm] * 4,
        out_specs=(vmem,) * 3,
        scratch_shapes=[
            pltpu.VMEM((2, ni + 2, nj + 2, nk + 2 * LEVEL, levels), jnp.float32),
            pltpu.VMEM((3, ni, nj, nk, levels), jnp.float32),
            pltpu.VMEM((n_south, ni, 2, nk, levels), jnp.float32),
            regular,
            regular,
            regular,
            dma((3,)),
            dma((2,)),
            dma((ni,)),
            dma((2, ni)),
            dma((2,)),
            dma((2, 2)),
            dma((sides, 2)),
            dma((2, sides, 2)),
            dma((others, 2)),
            dma((others, 2)),
        ],
        compiler_params=pltpu.CompilerParams(
            collective_id=0, has_side_effects=True, vmem_limit_bytes=46 * 2**20
        ),
    )(*(pltpu.with_memory_space_constraint(array, pltpu.HBM)
        for array in (field_values, flow_j, flow_i, flow_k)))
    pieces = 8
    return pl.pallas_call(
        functools.partial(scale, pieces),
        name="scale",
        in_specs=[vmem] * 3,
        out_specs=(hbm, hbm),
        out_shape=(whole, whole),
        scratch_shapes=[
            pltpu.VMEM(field_values.shape, jnp.float32),
            dma((pieces,)),
            dma((pieces,)),
        ],
        compiler_params=pltpu.CompilerParams(vmem_limit_bytes=16 * 2**20),
    )(end, mean, factor)


def solution(mesh):
    counts = tuple(mesh.shape[axis] for axis in ("south", "east", "down"))
    spec = P("south", "east", "down", None)
    return jax.shard_map(
        functools.partial(per_device, counts),
        mesh=mesh,
        in_specs=(spec,) * 4,
        out_specs=(spec, spec),
        check_vma=False,
    )
```

```python
import functools

import jax
import jax.numpy as jnp
from jax import lax
from jax.experimental import pallas as pl
from jax.experimental.pallas import tpu as pltpu
from jax.sharding import PartitionSpec as P

STEPS = 6
BLOCK = 8
LEVEL = 4
MESH = pl.DeviceIdType.MESH


def transport(counts, steps, field, flow_j, flow_i, flow_k, end, mean_out, scale_out,
              cells, flows, stats,
              ready_down, ready_east, ready_south, load_sem, flow_sem,
              k_send, k_recv, i_send, i_recv, j_send, j_recv, stat_send, stat_recv):
    n_south, n_east, n_down = counts
    nj, ni, nk, levels = field.shape
    inner = pl.ds(LEVEL, nk)
    blocks = nj // BLOCK
    half = ni // 2
    early = ni - 2
    south, east, down = (lax.axis_index(a) for a in ("south", "east", "down"))
    place = {"south": (south, n_south), "east": (east, n_east), "down": (down, n_down)}
    upward = lax.rem(east, 2) == 1

    def has(axis, side):
        me, count = place[axis]
        return me > 0 if side == 0 else me < count - 1

    def beside(axis, side):
        me, _ = place[axis]
        return {axis: me - 1 if side == 0 else me + 1}

    def row_of(turn):
        return jnp.where(upward, turn, ni - 1 - turn)

    def rows_of(first, count):
        return pl.ds(jnp.where(upward, first, ni - first - count), count)

    def load(turn):
        i = row_of(turn)
        return pltpu.make_async_copy(
            field.at[pl.ds(0, nj), i], cells.at[0, i + 1, pl.ds(1, nj), inner],
            load_sem.at[jnp.minimum(turn, 2)],
        )

    def loaded(first, count):
        start = jnp.where(upward, first, ni - first - count)
        part = cells.at[0, pl.ds(start + 1, count), pl.ds(1, nj), inner]
        pltpu.make_async_copy(part, part, load_sem.at[first]).wait()

    def load_flows(turn):
        i = row_of(turn)
        for d, source in enumerate((flow_j, flow_i, flow_k)):
            pltpu.make_async_copy(
                source.at[pl.ds(0, nj), i], flows.at[d, i], flow_sem.at[jnp.where(turn < 2, 0, 1)]
            ).start()

    def flows_loaded(group):
        rows = rows_of(0, 2) if group == 0 else rows_of(2, early)
        part = flows.at[pl.ds(0, 3), rows]
        pltpu.make_async_copy(part, part, flow_sem.at[group]).wait()

    def edge(side):
        return LEVEL if side == 0 else LEVEL + nk - 1

    def halo(side):
        return LEVEL - 1 if side == 0 else LEVEL + nk

    def k_copy(slot, side, i):
        part = pl.ds(1, nj)
        return pltpu.make_async_remote_copy(
            cells.at[slot, i + 1, part, edge(side)], cells.at[slot, i + 1, part, halo(1 - side)],
            k_send.at[i], k_recv.at[slot, i],
            device_id=beside("down", side), device_id_type=MESH,
        )

    def k_both(slot, i):
        part = cells.at[slot, i + 1, pl.ds(1, nj), pl.ds(LEVEL, 2)]
        return pltpu.make_async_remote_copy(
            part, part, k_send.at[i], k_recv.at[slot, i],
            device_id=beside("down", 0), device_id_type=MESH,
        )

    def i_copy(slot, side):
        part = pl.ds(1, nj)
        return pltpu.make_async_remote_copy(
            cells.at[slot, 1 if side == 0 else ni, part, inner],
            cells.at[slot, ni + 1 if side == 0 else 0, part, inner],
            i_send.at[side], i_recv.at[slot, 1 - side],
            device_id=beside("east", side), device_id_type=MESH,
        )

    def j_copy(slot, side, group):
        rows = pl.ds(jnp.where(upward, group * half, ni - (group + 1) * half) + 1, half)
        sending, receiving = (side, 1 - side) if n_south > 2 else (0, 0)
        return pltpu.make_async_remote_copy(
            cells.at[slot, rows, 1 if side == 0 else nj, inner],
            cells.at[slot, rows, nj + 1 if side == 0 else 0, inner],
            j_send.at[sending, group], j_recv.at[slot, receiving, group],
            device_id=beside("south", side), device_id_type=MESH,
        )

    def edge_turn(side):
        return jnp.where(upward == (side == 0), 0, ni - 1)

    def each_k(act):
        if n_down > 1:
            inside = has("down", 0) & has("down", 1)
            pl.when(inside)(lambda: act(k_both))
            pl.when(jnp.logical_not(inside))(lambda: act(lambda slot, i: k_copy(slot, 0, i)))

    def sent(slot, turn):
        each_k(lambda copy: copy(slot, row_of(turn)).wait_send())

    def received(slot, turn):
        each_k(lambda copy: copy(slot, row_of(turn)).wait_recv())
        for side in (0, 1):
            pl.when(has("east", side) & (turn == edge_turn(side)))(
                lambda: i_copy(slot, 1 - side).wait_recv())
        for group in (0, 1):
            for side in (0, 1):
                pl.when(has("south", side) & (turn == group * half))(
                    lambda: j_copy(slot, 1 - side, group).wait_recv())

    def send_k(slot, side, turn):
        pl.when(has("down", side))(lambda: k_copy(slot, side, row_of(turn)).start())

    def send(slot, turn, held):
        @pl.when(jnp.logical_not(held))
        def _():
            for side in (0, 1):
                send_k(slot, side, turn)

        @pl.when(held & (turn == ni - 1))
        def _():
            @pl.loop(0, ni)
            def _(other):
                for side in (0, 1):
                    send_k(slot, side, other)

        for side in (0, 1):
            @pl.when(has("east", side) & (turn == edge_turn(side)))
            def _():
                i_copy(slot, side).wait_send()
                i_copy(slot, side).start()
        for group in (0, 1):
            for side in (0, 1):
                @pl.when(has("south", side) & (turn == (group + 1) * half - 1))
                def _():
                    j_copy(slot, side, group).wait_send()
                    j_copy(slot, side, group).start()

    zero = jnp.zeros((nk, levels), jnp.float32)

    barrier = pltpu.get_barrier_semaphore()
    lower = south
    for offset in range(1, n_south):
        @pl.when(south + offset < n_south)
        def _():
            pl.semaphore_signal(barrier, 1, device_id={"south": south + offset},
                                device_id_type=MESH)
    for axis in ("down", "east"):
        lower = lower + has(axis, 0).astype(jnp.int32)

        @pl.when(has(axis, 1))
        def _():
            pl.semaphore_signal(barrier, 1, device_id=beside(axis, 1), device_id_type=MESH)

    @pl.loop(0, ni)
    def _(turn):
        load(turn).start()

    pl.when(lower > 0)(lambda: pl.semaphore_wait(barrier, lower))
    for axis, ready in (("down", ready_down), ("east", ready_east)):
        @pl.when(has(axis, 0))
        def _():
            pl.semaphore_signal(ready, 1, device_id=beside(axis, 0), device_id_type=MESH)
    for offset in range(1, n_south):
        @pl.when(south - offset >= 0)
        def _():
            pl.semaphore_signal(ready_south, 1, device_id={"south": south - offset},
                                device_id_type=MESH)

    for turn in (0, 1):
        loaded(turn, 1)
        send_k(0, 0, turn)
    pl.when(has("down", 1))(lambda: pl.semaphore_wait(ready_down, 1))
    for turn in (0, 1):
        send_k(0, 1, turn)
    loaded(2, early)

    @pl.loop(2, ni)
    def _(turn):
        for side in (0, 1):
            send_k(0, side, turn)

    @pl.loop(0, ni)
    def _(turn):
        load_flows(turn)

    pl.when(has("east", 1))(lambda: pl.semaphore_wait(ready_east, 1))
    for side in (0, 1):
        pl.when(has("east", side))(lambda: i_copy(0, side).start())
    if n_south > 1:
        pl.when(has("south", 1))(lambda: pl.semaphore_wait(ready_south, n_south - 1 - south))
    for group in (0, 1):
        for side in (0, 1):
            pl.when(has("south", side))(lambda: j_copy(0, side, group).start())

    for side in (0, 1):
        @pl.when(jnp.logical_not(has("down", side)))
        def _():
            @pl.loop(0, ni)
            def _(i):
                @pl.loop(0, blocks)
                def _(block):
                    for slot in (0, 1):
                        cells[slot, i + 1, pl.ds(block * BLOCK + 1, BLOCK), halo(side)] = (
                            jnp.zeros((BLOCK, levels), jnp.float32))

        @pl.when(jnp.logical_not(has("east", side)))
        def _():
            @pl.loop(0, nj)
            def _(j):
                for slot in (0, 1):
                    cells[slot, 0 if side == 0 else ni + 1, j + 1, inner] = zero

        @pl.when(jnp.logical_not(has("south", side)))
        def _():
            @pl.loop(0, ni)
            def _(i):
                for slot in (0, 1):
                    cells[slot, i + 1, 0 if side == 0 else nj + 1, inner] = zero

    def advanced(slot, i, j):
        here = pl.ds(j + 1, BLOCK)
        column = cells[slot, i + 1, pl.ds(j, BLOCK + 2), inner]
        middle = column[1:BLOCK + 1]
        sides = (
            (column[:BLOCK], column[2:]),
            (cells[slot, i, here, inner], cells[slot, i + 2, here, inner]),
            (cells[slot, i + 1, here, pl.ds(LEVEL - 1, nk)],
             cells[slot, i + 1, here, pl.ds(LEVEL + 1, nk)]),
        )
        around, drift = None, None
        for d, (low, high) in enumerate(sides):
            both = low + high
            moved = flows[d, i, pl.ds(j, BLOCK)] * (low - high)
            around = both if d == 0 else around + both
            drift = moved if d == 0 else drift + moved
        return (0.7 * middle + 0.05 * around) + drift

    @pl.loop(1, steps)
    def _(step):
        now, later = lax.rem(step + 1, 2), lax.rem(step, 2)

        @pl.loop(0, ni)
        def _(turn):
            i = row_of(turn)
            for group, first in enumerate((0, 2)):
                pl.when((step == 1) & (turn == first))(lambda: flows_loaded(group))
            sent(now, turn)
            received(now, turn)

            @pl.loop(0, blocks, unroll=2)
            def _(block):
                j = pl.multiple_of(block * BLOCK, BLOCK)
                values = advanced(now, i, j)
                cells[later, i + 1, pl.ds(j + 1, BLOCK), inner] = values

            send(later, turn, upward & (step == steps - 1))

    now = (steps - 1) % 2

    def stat_copy(offset, owner, part):
        target = lax.rem(south + offset, n_south)
        rows = rows_of(0, early) if part == 0 else rows_of(early, 2)
        return pltpu.make_async_remote_copy(
            stats.at[owner, rows], stats.at[owner, rows],
            stat_send.at[offset - 1, part], stat_recv.at[offset - 1, part],
            device_id={"south": target}, device_id_type=MESH,
        )

    @pl.loop(0, ni)
    def _(turn):
        i = row_of(turn)
        received(now, turn)

        def block(b, total):
            j = pl.multiple_of(b * BLOCK, BLOCK)
            values = advanced(now, i, j)
            end[pl.ds(j, BLOCK), i] = values
            return total + jnp.sum(values, axis=0)

        own_mean = lax.fori_loop(0, blocks, block, zero, unroll=2) * (1.0 / nj)

        def square(b, total):
            centred = end[pl.ds(b * BLOCK, BLOCK), i] - own_mean
            return total + jnp.sum(centred * centred, axis=0)

        stats[south, i, 0] = own_mean
        stats[south, i, 1] = lax.fori_loop(0, blocks, square, zero, unroll=2)
        for part, last in enumerate((early - 1, ni - 1)):
            @pl.when(turn == last)
            def _():
                for offset in range(1, n_south):
                    stat_copy(offset, south, part).start()

    @pl.loop(0, ni)
    def _(turn):
        sent(now, turn)

    for side in (0, 1):
        pl.when(has("east", side))(lambda: i_copy(now, side).wait_send())
        for group in (0, 1):
            pl.when(has("south", side))(lambda: j_copy(now, side, group).wait_send())

    for part, (first, count) in enumerate(((0, early), (early, 2))):
        for offset in range(1, n_south):
            owner = lax.rem(south + n_south - offset, n_south)
            stat_copy(offset, owner, part).wait_recv()

        @pl.loop(first, first + count)
        def _(turn):
            i = row_of(turn)
            whole_mean = stats[0, i, 0]
            for other in range(1, n_south):
                whole_mean = whole_mean + stats[other, i, 0]
            whole_mean = whole_mean * (1.0 / n_south)
            whole_squares = zero
            for other in range(n_south):
                away = stats[other, i, 0] - whole_mean
                whole_squares = whole_squares + (stats[other, i, 1] + nj * (away * away))
            mean_out[i] = whole_mean
            scale_out[i] = lax.rsqrt(whole_squares * (1.0 / (nj * n_south)) + 0.0001)

    for part in (0, 1):
        for offset in range(1, n_south):
            stat_copy(offset, south, part).wait_send()


def scale(pieces, values, mean, factor, standardized, copied, scaled, copy_sem, scale_sem):
    rows = values.shape[0] // pieces

    def copy_out(c):
        part = pl.ds(c * rows, rows)
        return pltpu.make_async_copy(values.at[part], copied.at[part], copy_sem.at[c])

    def scale_out(c):
        part = pl.ds(c * rows, rows)
        return pltpu.make_async_copy(scaled.at[part], standardized.at[part], scale_sem.at[c])

    @pl.loop(0, pieces)
    def _(c):
        copy_out(c).start()

    @pl.loop(0, pieces)
    def _(c):
        @pl.loop(0, rows)
        def _(offset):
            r = c * rows + offset
            scaled[r] = (values[r] - mean[...]) * factor[...]

        scale_out(c).start()

    @pl.loop(0, pieces)
    def _(c):
        copy_out(c).wait()
        scale_out(c).wait()


def per_device(counts, field_values, flow_j, flow_i, flow_k):
    nj, ni, nk, levels = field_values.shape
    n_south = counts[0]
    plane = (ni, nk, levels)
    whole = jax.ShapeDtypeStruct(field_values.shape, jnp.float32)
    vmem = pl.BlockSpec(memory_space=pltpu.VMEM)
    hbm = pl.BlockSpec(memory_space=pltpu.HBM)
    dma = pltpu.SemaphoreType.DMA
    regular = pltpu.SemaphoreType.REGULAR
    others = max(n_south - 1, 1)
    sides = 2 if n_south > 2 else 1
    end, mean, factor = pl.pallas_call(
        functools.partial(transport, counts, STEPS),
        name="transport",
        out_shape=(
            whole,
            jax.ShapeDtypeStruct(plane, jnp.float32),
            jax.ShapeDtypeStruct(plane, jnp.float32),
        ),
        in_specs=[hbm] * 4,
        out_specs=(vmem,) * 3,
        scratch_shapes=[
            pltpu.VMEM((2, ni + 2, nj + 2, nk + 2 * LEVEL, levels), jnp.float32),
            pltpu.VMEM((3, ni, nj, nk, levels), jnp.float32),
            pltpu.VMEM((n_south, ni, 2, nk, levels), jnp.float32),
            regular,
            regular,
            regular,
            dma((3,)),
            dma((2,)),
            dma((ni,)),
            dma((2, ni)),
            dma((2,)),
            dma((2, 2)),
            dma((sides, 2)),
            dma((2, sides, 2)),
            dma((others, 2)),
            dma((others, 2)),
        ],
        compiler_params=pltpu.CompilerParams(
            collective_id=0, has_side_effects=True, vmem_limit_bytes=46 * 2**20
        ),
    )(*(pltpu.with_memory_space_constraint(array, pltpu.HBM)
        for array in (field_values, flow_j, flow_i, flow_k)))
    pieces = 8
    return pl.pallas_call(
        functools.partial(scale, pieces),
        name="scale",
        in_specs=[vmem] * 3,
        out_specs=(hbm, hbm),
        out_shape=(whole, whole),
        scratch_shapes=[
            pltpu.VMEM(field_values.shape, jnp.float32),
            dma((pieces,)),
            dma((pieces,)),
        ],
        compiler_params=pltpu.CompilerParams(vmem_limit_bytes=16 * 2**20),
    )(end, mean, factor)


def solution(mesh):
    counts = tuple(mesh.shape[axis] for axis in ("south", "east", "down"))
    spec = P("south", "east", "down", None)
    return jax.shard_map(
        functools.partial(per_device, counts),
        mesh=mesh,
        in_specs=(spec,) * 4,
        out_specs=(spec, spec),
        check_vma=False,
    )
```

```python
import functools

import jax
import jax.numpy as jnp
from jax import lax
from jax.experimental import pallas as pl
from jax.experimental.pallas import tpu as pltpu
from jax.sharding import PartitionSpec as P

STEPS = 6
BLOCK = 8
LEVEL = 4
MESH = pl.DeviceIdType.MESH


def transport(counts, steps, field, flow_j, flow_i, flow_k, end, mean_out, scale_out,
              cells, flows, stats,
              ready_down, ready_east, ready_south, load_sem, flow_sem,
              k_send, k_recv, k_last, i_send, i_recv, j_send, j_recv, stat_send, stat_recv):
    n_south, n_east, n_down = counts
    nj, ni, nk, levels = field.shape
    inner = pl.ds(LEVEL, nk)
    blocks = nj // BLOCK
    half = ni // 2
    early = ni - 2
    south, east, down = (lax.axis_index(a) for a in ("south", "east", "down"))
    place = {"south": (south, n_south), "east": (east, n_east), "down": (down, n_down)}
    upward = lax.rem(east, 2) == 1

    def has(axis, side):
        me, count = place[axis]
        return me > 0 if side == 0 else me < count - 1

    def beside(axis, side):
        me, _ = place[axis]
        return {axis: me - 1 if side == 0 else me + 1}

    def row_of(turn):
        return jnp.where(upward, turn, ni - 1 - turn)

    def rows_of(first, count):
        return pl.ds(jnp.where(upward, first, ni - first - count), count)

    def load(turn):
        i = row_of(turn)
        return pltpu.make_async_copy(
            field.at[pl.ds(0, nj), i], cells.at[0, i + 1, pl.ds(1, nj), inner],
            load_sem.at[jnp.minimum(turn, 2)],
        )

    def load_edge(side):
        i = row_of(0)
        return pltpu.make_async_copy(
            field.at[pl.ds(0, nj), i, 0 if side == 0 else nk - 1],
            cells.at[0, i + 1, pl.ds(1, nj), edge(side)], load_sem.at[0])

    def edges_loaded():
        part = cells.at[0, row_of(0) + 1, pl.ds(1, nj), pl.ds(LEVEL, 2)]
        pltpu.make_async_copy(part, part, load_sem.at[0]).wait()

    def load_between():
        i = row_of(0)
        return pltpu.make_async_copy(
            field.at[pl.ds(0, nj), i, pl.ds(1, nk - 2)],
            cells.at[0, i + 1, pl.ds(1, nj), pl.ds(LEVEL + 1, nk - 2)], load_sem.at[0])

    def loaded(first, count):
        start = jnp.where(upward, first, ni - first - count)
        part = cells.at[0, pl.ds(start + 1, count), pl.ds(1, nj), inner]
        pltpu.make_async_copy(part, part, load_sem.at[first]).wait()

    def load_flows(turn):
        i = row_of(turn)
        for d, source in enumerate((flow_j, flow_i, flow_k)):
            pltpu.make_async_copy(
                source.at[pl.ds(0, nj), i], flows.at[d, i], flow_sem.at[jnp.where(turn < 2, 0, 1)]
            ).start()

    def flows_loaded(group):
        rows = rows_of(0, 2) if group == 0 else rows_of(2, early)
        part = flows.at[pl.ds(0, 3), rows]
        pltpu.make_async_copy(part, part, flow_sem.at[group]).wait()

    def edge(side):
        return LEVEL if side == 0 else LEVEL + nk - 1

    def halo(side):
        return LEVEL - 1 if side == 0 else LEVEL + nk

    def k_copy(slot, side, i):
        part = pl.ds(1, nj)
        return pltpu.make_async_remote_copy(
            cells.at[slot, i + 1, part, edge(side)], cells.at[slot, i + 1, part, halo(1 - side)],
            k_send.at[slot], k_recv.at[slot, i],
            device_id=beside("down", side), device_id_type=MESH,
        )

    def half_span(part):
        return pl.ds(1 + part * (nj // 2), nj // 2)

    def half_recv(slot, i, part):
        return k_recv.at[slot, i] if part == 0 else k_last

    def k_half(slot, side, i, part):
        return pltpu.make_async_remote_copy(
            cells.at[slot, i + 1, half_span(part), edge(side)],
            cells.at[slot, i + 1, half_span(part), halo(1 - side)],
            k_send.at[slot], half_recv(slot, i, part),
            device_id=beside("down", side), device_id_type=MESH,
        )

    def k_all(slot, rows, span, neighbours, arrival):
        part = cells.at[slot, rows, span, pl.ds(LEVEL, neighbours)]
        return pltpu.make_async_remote_copy(
            part, part, k_send.at[slot], arrival,
            device_id=beside("down", 0), device_id_type=MESH,
        )

    def i_copy(slot, side):
        part = pl.ds(1, nj)
        return pltpu.make_async_remote_copy(
            cells.at[slot, 1 if side == 0 else ni, part, inner],
            cells.at[slot, ni + 1 if side == 0 else 0, part, inner],
            i_send.at[side], i_recv.at[slot, 1 - side],
            device_id=beside("east", side), device_id_type=MESH,
        )

    def j_copy(slot, side, group):
        rows = pl.ds(jnp.where(upward, group * half, ni - (group + 1) * half) + 1, half)
        sending, receiving = (side, 1 - side) if n_south > 2 else (0, 0)
        return pltpu.make_async_remote_copy(
            cells.at[slot, rows, 1 if side == 0 else nj, inner],
            cells.at[slot, rows, nj + 1 if side == 0 else 0, inner],
            j_send.at[sending, group], j_recv.at[slot, receiving, group],
            device_id=beside("south", side), device_id_type=MESH,
        )

    def edge_turn(side):
        return jnp.where(upward == (side == 0), 0, ni - 1)

    def each_k(act):
        if n_down > 1:
            inside = has("down", 0) & has("down", 1)
            pl.when(inside)(lambda: act(2))
            pl.when(jnp.logical_not(inside))(lambda: act(1))

    def sent(slot):
        each_k(lambda count: k_all(
            slot, pl.ds(1, ni), pl.ds(1, nj), count, k_recv.at[slot, 0]).wait_send())

    def half_received(slot, turn, part):
        i = row_of(turn)
        each_k(lambda count: k_all(
            slot, pl.ds(i + 1, 1), half_span(part), count, half_recv(slot, i, part)).wait_recv())

    def received(slot, turn):
        i = row_of(turn)
        each_k(lambda count: k_all(
            slot, pl.ds(i + 1, 1), pl.ds(1, nj), count, k_recv.at[slot, i]).wait_recv())
        sides_received(slot, turn)

    def sides_received(slot, turn):
        for side in (0, 1):
            pl.when(has("east", side) & (turn == edge_turn(side)))(
                lambda: i_copy(slot, 1 - side).wait_recv())
        for group in (0, 1):
            for side in (0, 1):
                pl.when(has("south", side) & (turn == group * half))(
                    lambda: j_copy(slot, 1 - side, group).wait_recv())

    def send_k(slot, side, turn):
        pl.when(has("down", side))(lambda: k_copy(slot, side, row_of(turn)).start())

    def send(slot, turn, final):
        ending = final & (turn == ni - 1)

        @pl.when(jnp.logical_not(ending | (final & upward)))
        def _():
            for side in (0, 1):
                send_k(slot, side, turn)

        @pl.when(ending)
        def _():
            @pl.when(upward)
            def _():
                @pl.loop(0, ni - 1)
                def _(other):
                    for side in (0, 1):
                        send_k(slot, side, other)

            i = row_of(turn)
            for part in (0, 1):
                for side in (0, 1):
                    pl.when(has("down", side))(lambda: k_half(slot, side, i, part).start())


        for side in (0, 1):
            @pl.when(has("east", side) & (turn == edge_turn(side)))
            def _():
                i_copy(slot, side).wait_send()
                i_copy(slot, side).start()
        for group in (0, 1):
            for side in (0, 1):
                @pl.when(has("south", side) & (turn == (group + 1) * half - 1))
                def _():
                    j_copy(slot, side, group).wait_send()
                    j_copy(slot, side, group).start()

    zero = jnp.zeros((nk, levels), jnp.float32)

    barrier = pltpu.get_barrier_semaphore()
    lower = south
    for offset in range(1, n_south):
        @pl.when(south + offset < n_south)
        def _():
            pl.semaphore_signal(barrier, 1, device_id={"south": south + offset},
                                device_id_type=MESH)
    lower = lower + has("down", 0).astype(jnp.int32)

    @pl.when(has("down", 1))
    def _():
        pl.semaphore_signal(barrier, 1, device_id=beside("down", 1), device_id_type=MESH)

    easts = jnp.int32(0)
    for side in (0, 1):
        easts = easts + has("east", side).astype(jnp.int32)

        @pl.when(upward & has("east", side))
        def _():
            pl.semaphore_signal(barrier, 1, device_id=beside("east", side), device_id_type=MESH)
    lower = lower + jnp.where(upward, 0, easts)

    for side in (0, 1):
        load_edge(side).start()

    @pl.loop(1, ni)
    def _(turn):
        load(turn).start()

    pl.when(lower > 0)(lambda: pl.semaphore_wait(barrier, lower))

    @pl.when(has("down", 0))
    def _():
        pl.semaphore_signal(ready_down, 1, device_id=beside("down", 0), device_id_type=MESH)

    for side in (0, 1):
        @pl.when(jnp.logical_not(upward) & has("east", side))
        def _():
            pl.semaphore_signal(ready_east, 1, device_id=beside("east", side),
                                device_id_type=MESH)
    for offset in range(1, n_south):
        @pl.when(south - offset >= 0)
        def _():
            pl.semaphore_signal(ready_south, 1, device_id={"south": south - offset},
                                device_id_type=MESH)

    edges_loaded()
    send_k(0, 0, 0)
    load_between().start()
    loaded(1, 1)
    send_k(0, 0, 1)
    pl.when(has("down", 1))(lambda: pl.semaphore_wait(ready_down, 1))
    for turn in (0, 1):
        send_k(0, 1, turn)
    loaded(2, early)
    load_between().wait()

    @pl.loop(2, ni)
    def _(turn):
        for side in (0, 1):
            send_k(0, side, turn)

    @pl.loop(0, ni)
    def _(turn):
        load_flows(turn)

    pl.when(upward & (easts > 0))(lambda: pl.semaphore_wait(ready_east, easts))
    for side in (0, 1):
        pl.when(has("east", side))(lambda: i_copy(0, side).start())
    if n_south > 1:
        pl.when(has("south", 1))(lambda: pl.semaphore_wait(ready_south, n_south - 1 - south))
    for group in (0, 1):
        for side in (0, 1):
            pl.when(has("south", side))(lambda: j_copy(0, side, group).start())

    for side in (0, 1):
        @pl.when(jnp.logical_not(has("down", side)))
        def _():
            @pl.loop(0, ni)
            def _(i):
                @pl.loop(0, blocks)
                def _(block):
                    for slot in (0, 1):
                        cells[slot, i + 1, pl.ds(block * BLOCK + 1, BLOCK), halo(side)] = (
                            jnp.zeros((BLOCK, levels), jnp.float32))

        @pl.when(jnp.logical_not(has("east", side)))
        def _():
            @pl.loop(0, nj)
            def _(j):
                for slot in (0, 1):
                    cells[slot, 0 if side == 0 else ni + 1, j + 1, inner] = zero

        @pl.when(jnp.logical_not(has("south", side)))
        def _():
            @pl.loop(0, ni)
            def _(i):
                for slot in (0, 1):
                    cells[slot, i + 1, 0 if side == 0 else nj + 1, inner] = zero

    def advanced(slot, i, j):
        here = pl.ds(j + 1, BLOCK)
        column = cells[slot, i + 1, pl.ds(j, BLOCK + 2), inner]
        middle = column[1:BLOCK + 1]
        sides = (
            (column[:BLOCK], column[2:]),
            (cells[slot, i, here, inner], cells[slot, i + 2, here, inner]),
            (cells[slot, i + 1, here, pl.ds(LEVEL - 1, nk)],
             cells[slot, i + 1, here, pl.ds(LEVEL + 1, nk)]),
        )
        around, drift = None, None
        for d, (low, high) in enumerate(sides):
            both = low + high
            moved = flows[d, i, pl.ds(j, BLOCK)] * (low - high)
            around = both if d == 0 else around + both
            drift = moved if d == 0 else drift + moved
        return (0.7 * middle + 0.05 * around) + drift

    @pl.loop(1, steps)
    def _(step):
        now, later = lax.rem(step + 1, 2), lax.rem(step, 2)

        @pl.loop(0, ni)
        def _(turn):
            i = row_of(turn)
            for group, first in enumerate((0, 2)):
                pl.when((step == 1) & (turn == first))(lambda: flows_loaded(group))
            pl.when((step >= 2) & (turn == 0))(lambda: sent(later))
            received(now, turn)

            @pl.loop(0, blocks, unroll=2)
            def _(block):
                j = pl.multiple_of(block * BLOCK, BLOCK)
                values = advanced(now, i, j)
                cells[later, i + 1, pl.ds(j + 1, BLOCK), inner] = values

            send(later, turn, step == steps - 1)

    now = (steps - 1) % 2

    def stat_copy(offset, owner, part):
        target = lax.rem(south + offset, n_south)
        rows = rows_of(0, early) if part == 0 else rows_of(early, 2)
        return pltpu.make_async_remote_copy(
            stats.at[owner, rows], stats.at[owner, rows],
            stat_send.at[offset - 1], stat_recv.at[offset - 1, part],
            device_id={"south": target}, device_id_type=MESH,
        )

    def finish(turn, waits):
        i = row_of(turn)

        def block(b, total):
            j = pl.multiple_of(b * BLOCK, BLOCK)
            values = advanced(now, i, j)
            end[pl.ds(j, BLOCK), i] = values
            return total + jnp.sum(values, axis=0)

        total = zero
        count = blocks // len(waits)
        for part, wait in enumerate(waits):
            wait()
            total = lax.fori_loop(part * count, (part + 1) * count, block, total, unroll=2)
        own_mean = total * (1.0 / nj)

        def square(b, total):
            centred = end[pl.ds(b * BLOCK, BLOCK), i] - own_mean
            return total + jnp.sum(centred * centred, axis=0)

        stats[south, i, 0] = own_mean
        stats[south, i, 1] = lax.fori_loop(0, blocks, square, zero, unroll=2)

    def send_stats(part):
        for offset in range(1, n_south):
            stat_copy(offset, south, part).start()

    @pl.loop(0, ni - 1)
    def _(turn):
        finish(turn, [lambda: received(now, turn)])
        pl.when(turn == early - 1)(lambda: send_stats(0))

    sides_received(now, ni - 1)
    finish(ni - 1, [lambda: half_received(now, ni - 1, 0), lambda: half_received(now, ni - 1, 1)])
    send_stats(1)

    for slot in (0, 1):
        sent(slot)
    for side in (0, 1):
        pl.when(has("east", side))(lambda: i_copy(now, side).wait_send())
        for group in (0, 1):
            pl.when(has("south", side))(lambda: j_copy(now, side, group).wait_send())

    for part, (first, count) in enumerate(((0, early), (early, 2))):
        for offset in range(1, n_south):
            owner = lax.rem(south + n_south - offset, n_south)
            stat_copy(offset, owner, part).wait_recv()

        @pl.loop(first, first + count)
        def _(turn):
            i = row_of(turn)
            whole_mean = stats[0, i, 0]
            for other in range(1, n_south):
                whole_mean = whole_mean + stats[other, i, 0]
            whole_mean = whole_mean * (1.0 / n_south)
            whole_squares = zero
            for other in range(n_south):
                away = stats[other, i, 0] - whole_mean
                whole_squares = whole_squares + (stats[other, i, 1] + nj * (away * away))
            mean_out[i] = whole_mean
            scale_out[i] = lax.rsqrt(whole_squares * (1.0 / (nj * n_south)) + 0.0001)

    for offset in range(1, n_south):
        whole = stats.at[south]
        pltpu.make_async_copy(whole, whole, stat_send.at[offset - 1]).wait()


def scale(pieces, values, mean, factor, standardized, copied, scaled, copy_sem, scale_sem):
    rows = values.shape[0] // pieces

    def copy_out(c):
        part = pl.ds(c * rows, rows)
        return pltpu.make_async_copy(values.at[part], copied.at[part], copy_sem)

    def scale_out(c):
        part = pl.ds(c * rows, rows)
        return pltpu.make_async_copy(scaled.at[part], standardized.at[part], scale_sem)

    @pl.loop(0, pieces)
    def _(c):
        copy_out(c).start()

    @pl.loop(0, pieces)
    def _(c):
        @pl.loop(0, rows)
        def _(offset):
            r = c * rows + offset
            scaled[r] = (values[r] - mean[...]) * factor[...]

        scale_out(c).start()

    pltpu.make_async_copy(values, copied, copy_sem).wait()
    pltpu.make_async_copy(scaled, standardized, scale_sem).wait()


def per_device(counts, field_values, flow_j, flow_i, flow_k):
    nj, ni, nk, levels = field_values.shape
    n_south = counts[0]
    plane = (ni, nk, levels)
    whole = jax.ShapeDtypeStruct(field_values.shape, jnp.float32)
    vmem = pl.BlockSpec(memory_space=pltpu.VMEM)
    hbm = pl.BlockSpec(memory_space=pltpu.HBM)
    dma = pltpu.SemaphoreType.DMA
    regular = pltpu.SemaphoreType.REGULAR
    others = max(n_south - 1, 1)
    sides = 2 if n_south > 2 else 1
    end, mean, factor = pl.pallas_call(
        functools.partial(transport, counts, STEPS),
        name="transport",
        out_shape=(
            whole,
            jax.ShapeDtypeStruct(plane, jnp.float32),
            jax.ShapeDtypeStruct(plane, jnp.float32),
        ),
        in_specs=[hbm] * 4,
        out_specs=(vmem,) * 3,
        scratch_shapes=[
            pltpu.VMEM((2, ni + 2, nj + 2, nk + 2 * LEVEL, levels), jnp.float32),
            pltpu.VMEM((3, ni, nj, nk, levels), jnp.float32),
            pltpu.VMEM((n_south, ni, 2, nk, levels), jnp.float32),
            regular,
            regular,
            regular,
            dma((3,)),
            dma((2,)),
            dma((2,)),
            dma((2, ni)),
            dma,
            dma((2,)),
            dma((2, 2)),
            dma((sides, 2)),
            dma((2, sides, 2)),
            dma((others,)),
            dma((others, 2)),
        ],
        compiler_params=pltpu.CompilerParams(
            collective_id=0, has_side_effects=True, vmem_limit_bytes=46 * 2**20
        ),
    )(*(pltpu.with_memory_space_constraint(array, pltpu.HBM)
        for array in (field_values, flow_j, flow_i, flow_k)))
    pieces = 4
    return pl.pallas_call(
        functools.partial(scale, pieces),
        name="scale",
        in_specs=[vmem] * 3,
        out_specs=(hbm, hbm),
        out_shape=(whole, whole),
        scratch_shapes=[
            pltpu.VMEM(field_values.shape, jnp.float32),
            dma,
            dma,
        ],
        compiler_params=pltpu.CompilerParams(vmem_limit_bytes=16 * 2**20),
    )(end, mean, factor)


def solution(mesh):
    counts = tuple(mesh.shape[axis] for axis in ("south", "east", "down"))
    spec = P("south", "east", "down", None)
    return jax.shard_map(
        functools.partial(per_device, counts),
        mesh=mesh,
        in_specs=(spec,) * 4,
        out_specs=(spec, spec),
        check_vma=False,
    )
```

```python
import functools

import jax
import jax.numpy as jnp
from jax import lax
from jax.experimental import pallas as pl
from jax.experimental.pallas import tpu as pltpu
from jax.sharding import PartitionSpec as P

STEPS = 6
BLOCK = 8
LEVEL = 4
MESH = pl.DeviceIdType.MESH


def transport(counts, steps, field, flow_j, flow_i, flow_k, end, mean_out, scale_out,
              cells, flows, stats,
              ready_down, ready_east, ready_south, load_sem, flow_sem,
              k_send, k_recv, k_last, i_send, i_recv, j_send, j_recv, stat_send, stat_recv):
    n_south, n_east, n_down = counts
    nj, ni, nk, levels = field.shape
    inner = pl.ds(LEVEL, nk)
    blocks = nj // BLOCK
    half = ni // 2
    early = ni - 2
    south, east, down = (lax.axis_index(a) for a in ("south", "east", "down"))
    place = {"south": (south, n_south), "east": (east, n_east), "down": (down, n_down)}
    upward = lax.rem(east, 2) == 1

    def has(axis, side):
        me, count = place[axis]
        return me > 0 if side == 0 else me < count - 1

    def beside(axis, side):
        me, _ = place[axis]
        return {axis: me - 1 if side == 0 else me + 1}

    def row_of(turn):
        return jnp.where(upward, turn, ni - 1 - turn)

    def rows_of(first, count):
        return pl.ds(jnp.where(upward, first, ni - first - count), count)

    def load(turn):
        i = row_of(turn)
        return pltpu.make_async_copy(
            field.at[pl.ds(0, nj), i], cells.at[0, i + 1, pl.ds(1, nj), inner],
            load_sem.at[jnp.minimum(turn, 2)],
        )

    def load_edge(side):
        i = row_of(0)
        return pltpu.make_async_copy(
            field.at[pl.ds(0, nj), i, 0 if side == 0 else nk - 1],
            cells.at[0, i + 1, pl.ds(1, nj), edge(side)], load_sem.at[0])

    def edges_loaded():
        part = cells.at[0, row_of(0) + 1, pl.ds(1, nj), pl.ds(LEVEL, 2)]
        pltpu.make_async_copy(part, part, load_sem.at[0]).wait()

    def load_between():
        i = row_of(0)
        return pltpu.make_async_copy(
            field.at[pl.ds(0, nj), i, pl.ds(1, nk - 2)],
            cells.at[0, i + 1, pl.ds(1, nj), pl.ds(LEVEL + 1, nk - 2)], load_sem.at[0])

    def loaded(first, count):
        start = jnp.where(upward, first, ni - first - count)
        part = cells.at[0, pl.ds(start + 1, count), pl.ds(1, nj), inner]
        pltpu.make_async_copy(part, part, load_sem.at[first]).wait()

    def load_flows(turn):
        i = row_of(turn)
        for d, source in enumerate((flow_j, flow_i, flow_k)):
            pltpu.make_async_copy(
                source.at[pl.ds(0, nj), i], flows.at[d, i], flow_sem.at[jnp.where(turn < 2, 0, 1)]
            ).start()

    def flows_loaded(group):
        rows = rows_of(0, 2) if group == 0 else rows_of(2, early)
        part = flows.at[pl.ds(0, 3), rows]
        pltpu.make_async_copy(part, part, flow_sem.at[group]).wait()

    def edge(side):
        return LEVEL if side == 0 else LEVEL + nk - 1

    def halo(side):
        return LEVEL - 1 if side == 0 else LEVEL + nk

    def k_copy(slot, side, i):
        part = pl.ds(1, nj)
        return pltpu.make_async_remote_copy(
            cells.at[slot, i + 1, part, edge(side)], cells.at[slot, i + 1, part, halo(1 - side)],
            k_send.at[slot], k_recv.at[slot, i],
            device_id=beside("down", side), device_id_type=MESH,
        )

    def half_span(part):
        return pl.ds(1 + part * (nj // 2), nj // 2)

    def half_recv(slot, i, part):
        return k_recv.at[slot, i] if part == 0 else k_last

    def k_half(slot, side, i, part):
        return pltpu.make_async_remote_copy(
            cells.at[slot, i + 1, half_span(part), edge(side)],
            cells.at[slot, i + 1, half_span(part), halo(1 - side)],
            k_send.at[slot], half_recv(slot, i, part),
            device_id=beside("down", side), device_id_type=MESH,
        )

    def k_all(slot, rows, span, neighbours, arrival):
        part = cells.at[slot, rows, span, pl.ds(LEVEL, neighbours)]
        return pltpu.make_async_remote_copy(
            part, part, k_send.at[slot], arrival,
            device_id=beside("down", 0), device_id_type=MESH,
        )

    def i_copy(slot, side):
        part = pl.ds(1, nj)
        return pltpu.make_async_remote_copy(
            cells.at[slot, 1 if side == 0 else ni, part, inner],
            cells.at[slot, ni + 1 if side == 0 else 0, part, inner],
            i_send.at[side], i_recv.at[slot, 1 - side],
            device_id=beside("east", side), device_id_type=MESH,
        )

    def j_copy(slot, side, group):
        rows = pl.ds(jnp.where(upward, group * half, ni - (group + 1) * half) + 1, half)
        sending, receiving = (side, 1 - side) if n_south > 2 else (0, 0)
        return pltpu.make_async_remote_copy(
            cells.at[slot, rows, 1 if side == 0 else nj, inner],
            cells.at[slot, rows, nj + 1 if side == 0 else 0, inner],
            j_send.at[sending, group], j_recv.at[slot, receiving, group],
            device_id=beside("south", side), device_id_type=MESH,
        )

    def edge_turn(side):
        return jnp.where(upward == (side == 0), 0, ni - 1)

    def each_k(act):
        if n_down > 1:
            inside = has("down", 0) & has("down", 1)
            pl.when(inside)(lambda: act(2))
            pl.when(jnp.logical_not(inside))(lambda: act(1))

    def sent(slot):
        each_k(lambda count: k_all(
            slot, pl.ds(1, ni), pl.ds(1, nj), count, k_recv.at[slot, 0]).wait_send())

    def half_received(slot, turn, part):
        i = row_of(turn)
        each_k(lambda count: k_all(
            slot, pl.ds(i + 1, 1), half_span(part), count, half_recv(slot, i, part)).wait_recv())

    def received(slot, turn):
        i = row_of(turn)
        each_k(lambda count: k_all(
            slot, pl.ds(i + 1, 1), pl.ds(1, nj), count, k_recv.at[slot, i]).wait_recv())
        sides_received(slot, turn)

    def sides_received(slot, turn):
        for side in (0, 1):
            pl.when(has("east", side) & (turn == edge_turn(side)))(
                lambda: i_copy(slot, 1 - side).wait_recv())
        for group in (0, 1):
            for side in (0, 1):
                pl.when(has("south", side) & (turn == group * half))(
                    lambda: j_copy(slot, 1 - side, group).wait_recv())

    def send_k(slot, side, turn):
        pl.when(has("down", side))(lambda: k_copy(slot, side, row_of(turn)).start())

    def send(slot, turn, final):
        ending = final & (turn == ni - 1)

        @pl.when(jnp.logical_not(ending | (final & upward)))
        def _():
            for side in (0, 1):
                send_k(slot, side, turn)

        @pl.when(ending)
        def _():
            @pl.when(upward)
            def _():
                @pl.loop(0, ni - 1)
                def _(other):
                    for side in (0, 1):
                        send_k(slot, side, other)

            i = row_of(turn)
            for part in (0, 1):
                for side in (0, 1):
                    pl.when(has("down", side))(lambda: k_half(slot, side, i, part).start())


        for side in (0, 1):
            @pl.when(has("east", side) & (turn == edge_turn(side)))
            def _():
                i_copy(slot, side).wait_send()
                i_copy(slot, side).start()
        for group in (0, 1):
            for side in (0, 1):
                @pl.when(has("south", side) & (turn == (group + 1) * half - 1))
                def _():
                    j_copy(slot, side, group).wait_send()
                    j_copy(slot, side, group).start()

    zero = jnp.zeros((nk, levels), jnp.float32)

    barrier = pltpu.get_barrier_semaphore()
    lower = south
    for offset in range(1, n_south):
        @pl.when(south + offset < n_south)
        def _():
            pl.semaphore_signal(barrier, 1, device_id={"south": south + offset},
                                device_id_type=MESH)
    lower = lower + has("down", 0).astype(jnp.int32)

    @pl.when(has("down", 1))
    def _():
        pl.semaphore_signal(barrier, 1, device_id=beside("down", 1), device_id_type=MESH)

    easts = jnp.int32(0)
    for side in (0, 1):
        easts = easts + has("east", side).astype(jnp.int32)

        @pl.when(upward & has("east", side))
        def _():
            pl.semaphore_signal(barrier, 1, device_id=beside("east", side), device_id_type=MESH)
    lower = lower + jnp.where(upward, 0, easts)

    for side in (0, 1):
        load_edge(side).start()

    @pl.loop(1, ni)
    def _(turn):
        load(turn).start()

    pl.when(lower > 0)(lambda: pl.semaphore_wait(barrier, lower))

    @pl.when(has("down", 0))
    def _():
        pl.semaphore_signal(ready_down, 1, device_id=beside("down", 0), device_id_type=MESH)

    for side in (0, 1):
        @pl.when(jnp.logical_not(upward) & has("east", side))
        def _():
            pl.semaphore_signal(ready_east, 1, device_id=beside("east", side),
                                device_id_type=MESH)
    for offset in range(1, n_south):
        @pl.when(south - offset >= 0)
        def _():
            pl.semaphore_signal(ready_south, 1, device_id={"south": south - offset},
                                device_id_type=MESH)

    edges_loaded()
    send_k(0, 0, 0)
    load_between().start()
    loaded(1, 1)
    send_k(0, 0, 1)
    pl.when(has("down", 1))(lambda: pl.semaphore_wait(ready_down, 1))
    for turn in (0, 1):
        send_k(0, 1, turn)
    loaded(2, early)
    load_between().wait()

    @pl.loop(2, ni)
    def _(turn):
        for side in (0, 1):
            send_k(0, side, turn)

    @pl.loop(0, ni)
    def _(turn):
        load_flows(turn)

    pl.when(upward & (easts > 0))(lambda: pl.semaphore_wait(ready_east, easts))
    for side in (0, 1):
        pl.when(has("east", side))(lambda: i_copy(0, side).start())
    if n_south > 1:
        pl.when(has("south", 1))(lambda: pl.semaphore_wait(ready_south, n_south - 1 - south))
    for group in (0, 1):
        for side in (0, 1):
            pl.when(has("south", side))(lambda: j_copy(0, side, group).start())

    for side in (0, 1):
        @pl.when(jnp.logical_not(has("down", side)))
        def _():
            @pl.loop(0, ni)
            def _(i):
                @pl.loop(0, blocks)
                def _(block):
                    for slot in (0, 1):
                        cells[slot, i + 1, pl.ds(block * BLOCK + 1, BLOCK), halo(side)] = (
                            jnp.zeros((BLOCK, levels), jnp.float32))

        @pl.when(jnp.logical_not(has("east", side)))
        def _():
            @pl.loop(0, nj)
            def _(j):
                for slot in (0, 1):
                    cells[slot, 0 if side == 0 else ni + 1, j + 1, inner] = zero

        @pl.when(jnp.logical_not(has("south", side)))
        def _():
            @pl.loop(0, ni)
            def _(i):
                for slot in (0, 1):
                    cells[slot, i + 1, 0 if side == 0 else nj + 1, inner] = zero

    def advanced(slot, i, j):
        here = pl.ds(j + 1, BLOCK)
        column = cells[slot, i + 1, pl.ds(j, BLOCK + 2), inner]
        middle = column[1:BLOCK + 1]
        sides = (
            (column[:BLOCK], column[2:]),
            (cells[slot, i, here, inner], cells[slot, i + 2, here, inner]),
            (cells[slot, i + 1, here, pl.ds(LEVEL - 1, nk)],
             cells[slot, i + 1, here, pl.ds(LEVEL + 1, nk)]),
        )
        above, moved = None, None
        for d, (low, high) in enumerate(sides):
            share = flows[d, i, pl.ds(j, BLOCK)] * (low - high)
            above = high if d == 0 else above + high
            moved = share if d == 0 else moved + share
        return (0.7 * middle + 0.1 * above) + moved

    def raise_flows(i):
        @pl.loop(0, blocks)
        def _(block):
            here = pl.ds(pl.multiple_of(block * BLOCK, BLOCK), BLOCK)
            for d in range(3):
                flows[d, i, here] = flows[d, i, here] + 0.05

    @pl.loop(1, steps)
    def _(step):
        now, later = lax.rem(step + 1, 2), lax.rem(step, 2)

        @pl.loop(0, ni)
        def _(turn):
            i = row_of(turn)
            for group, first in enumerate((0, 2)):
                pl.when((step == 1) & (turn == first))(lambda: flows_loaded(group))
            pl.when(step == 1)(lambda: raise_flows(i))
            pl.when((step >= 2) & (turn == 0))(lambda: sent(later))
            received(now, turn)

            @pl.loop(0, blocks, unroll=2)
            def _(block):
                j = pl.multiple_of(block * BLOCK, BLOCK)
                values = advanced(now, i, j)
                cells[later, i + 1, pl.ds(j + 1, BLOCK), inner] = values

            send(later, turn, step == steps - 1)

    now = (steps - 1) % 2

    def stat_copy(offset, owner, part):
        target = lax.rem(south + offset, n_south)
        rows = rows_of(0, early) if part == 0 else rows_of(early, 2)
        return pltpu.make_async_remote_copy(
            stats.at[owner, rows], stats.at[owner, rows],
            stat_send.at[offset - 1], stat_recv.at[offset - 1, part],
            device_id={"south": target}, device_id_type=MESH,
        )

    def finish(turn, waits):
        i = row_of(turn)

        def store(j):
            values = advanced(now, i, j)
            end[pl.ds(j, BLOCK), i] = values
            return values

        def block(b, sums):
            away = store(pl.multiple_of(b * BLOCK, BLOCK)) - shift
            return sums[0] + jnp.sum(away, axis=0), sums[1] + jnp.sum(away * away, axis=0)

        count = blocks // len(waits)
        for part, wait in enumerate(waits):
            wait()
            first = part * count
            if part == 0:
                start = [store(b * BLOCK) for b in range(2)]
                shift = jnp.sum(start[0] + start[1], axis=0) * (0.5 / BLOCK)
                away = [values - shift for values in start]
                sums = (jnp.sum(away[0] + away[1], axis=0),
                        jnp.sum(away[0] * away[0] + away[1] * away[1], axis=0))
                first = 2
            sums = lax.fori_loop(first, (part + 1) * count, block, sums, unroll=2)
        stats[south, i, 0] = shift + sums[0] * (1.0 / nj)
        stats[south, i, 1] = jnp.maximum(sums[1] - sums[0] * sums[0] * (1.0 / nj), 0.0)

    def send_stats(part):
        for offset in range(1, n_south):
            stat_copy(offset, south, part).start()

    @pl.loop(0, ni - 1)
    def _(turn):
        finish(turn, [lambda: received(now, turn)])
        pl.when(turn == early - 1)(lambda: send_stats(0))

    sides_received(now, ni - 1)
    finish(ni - 1, [lambda: half_received(now, ni - 1, 0), lambda: half_received(now, ni - 1, 1)])
    send_stats(1)

    for slot in (0, 1):
        sent(slot)
    for side in (0, 1):
        pl.when(has("east", side))(lambda: i_copy(now, side).wait_send())
        for group in (0, 1):
            pl.when(has("south", side))(lambda: j_copy(now, side, group).wait_send())

    for part, (first, count) in enumerate(((0, early), (early, 2))):
        for offset in range(1, n_south):
            owner = lax.rem(south + n_south - offset, n_south)
            stat_copy(offset, owner, part).wait_recv()

        @pl.loop(first, first + count)
        def _(turn):
            i = row_of(turn)
            whole_mean = stats[0, i, 0]
            for other in range(1, n_south):
                whole_mean = whole_mean + stats[other, i, 0]
            whole_mean = whole_mean * (1.0 / n_south)
            whole_squares = zero
            for other in range(n_south):
                away = stats[other, i, 0] - whole_mean
                whole_squares = whole_squares + (stats[other, i, 1] + nj * (away * away))
            mean_out[i] = whole_mean
            scale_out[i] = lax.rsqrt(whole_squares * (1.0 / (nj * n_south)) + 0.0001)

    for offset in range(1, n_south):
        whole = stats.at[south]
        pltpu.make_async_copy(whole, whole, stat_send.at[offset - 1]).wait()


def scale(pieces, values, mean, factor, standardized, copied, scaled, copy_sem, scale_sem):
    rows = values.shape[0] // pieces

    def copy_out(c):
        part = pl.ds(c * rows, rows)
        return pltpu.make_async_copy(values.at[part], copied.at[part], copy_sem)

    def scale_out(c):
        part = pl.ds(c * rows, rows)
        return pltpu.make_async_copy(scaled.at[part], standardized.at[part], scale_sem)

    @pl.loop(0, pieces)
    def _(c):
        copy_out(c).start()

    @pl.loop(0, pieces)
    def _(c):
        @pl.loop(0, rows)
        def _(offset):
            r = c * rows + offset
            scaled[r] = (values[r] - mean[...]) * factor[...]

        scale_out(c).start()

    pltpu.make_async_copy(values, copied, copy_sem).wait()
    pltpu.make_async_copy(scaled, standardized, scale_sem).wait()


def per_device(counts, field_values, flow_j, flow_i, flow_k):
    nj, ni, nk, levels = field_values.shape
    n_south = counts[0]
    plane = (ni, nk, levels)
    whole = jax.ShapeDtypeStruct(field_values.shape, jnp.float32)
    vmem = pl.BlockSpec(memory_space=pltpu.VMEM)
    hbm = pl.BlockSpec(memory_space=pltpu.HBM)
    dma = pltpu.SemaphoreType.DMA
    regular = pltpu.SemaphoreType.REGULAR
    others = max(n_south - 1, 1)
    sides = 2 if n_south > 2 else 1
    end, mean, factor = pl.pallas_call(
        functools.partial(transport, counts, STEPS),
        name="transport",
        out_shape=(
            whole,
            jax.ShapeDtypeStruct(plane, jnp.float32),
            jax.ShapeDtypeStruct(plane, jnp.float32),
        ),
        in_specs=[hbm] * 4,
        out_specs=(vmem,) * 3,
        scratch_shapes=[
            pltpu.VMEM((2, ni + 2, nj + 2, nk + 2 * LEVEL, levels), jnp.float32),
            pltpu.VMEM((3, ni, nj, nk, levels), jnp.float32),
            pltpu.VMEM((n_south, ni, 2, nk, levels), jnp.float32),
            regular,
            regular,
            regular,
            dma((3,)),
            dma((2,)),
            dma((2,)),
            dma((2, ni)),
            dma,
            dma((2,)),
            dma((2, 2)),
            dma((sides, 2)),
            dma((2, sides, 2)),
            dma((others,)),
            dma((others, 2)),
        ],
        compiler_params=pltpu.CompilerParams(
            collective_id=0, has_side_effects=True, vmem_limit_bytes=46 * 2**20
        ),
    )(*(pltpu.with_memory_space_constraint(array, pltpu.HBM)
        for array in (field_values, flow_j, flow_i, flow_k)))
    pieces = 4
    return pl.pallas_call(
        functools.partial(scale, pieces),
        name="scale",
        in_specs=[vmem] * 3,
        out_specs=(hbm, hbm),
        out_shape=(whole, whole),
        scratch_shapes=[
            pltpu.VMEM(field_values.shape, jnp.float32),
            dma,
            dma,
        ],
        compiler_params=pltpu.CompilerParams(vmem_limit_bytes=16 * 2**20),
    )(end, mean, factor)


def solution(mesh):
    counts = tuple(mesh.shape[axis] for axis in ("south", "east", "down"))
    spec = P("south", "east", "down", None)
    return jax.shard_map(
        functools.partial(per_device, counts),
        mesh=mesh,
        in_specs=(spec,) * 4,
        out_specs=(spec, spec),
        check_vma=False,
    )
```

```python
import functools

import jax
import jax.numpy as jnp
from jax import lax
from jax.experimental import pallas as pl
from jax.experimental.pallas import tpu as pltpu
from jax.sharding import PartitionSpec as P

STEPS = 6
BLOCK = 8
LEVEL = 4
MESH = pl.DeviceIdType.MESH


def transport(counts, steps, field, flow_j, flow_i, flow_k, end, mean_out, scale_out,
              cells, flows, stats,
              ready_down, ready_east, ready_south, load_sem, flow_sem,
              k_send, k_recv, k_last, i_send, i_recv, j_send, j_recv, stat_send, stat_recv):
    n_south, n_east, n_down = counts
    nj, ni, nk, levels = field.shape
    inner = pl.ds(LEVEL, nk)
    blocks = nj // BLOCK
    half = ni // 2
    early = ni - 2
    south, east, down = (lax.axis_index(a) for a in ("south", "east", "down"))
    place = {"south": (south, n_south), "east": (east, n_east), "down": (down, n_down)}
    upward = lax.rem(east, 2) == 1

    def has(axis, side):
        me, count = place[axis]
        return me > 0 if side == 0 else me < count - 1

    def beside(axis, side):
        me, _ = place[axis]
        return {axis: me - 1 if side == 0 else me + 1}

    def row_of(turn):
        return jnp.where(upward, turn, ni - 1 - turn)

    def rows_of(first, count):
        return pl.ds(jnp.where(upward, first, ni - first - count), count)

    def load(turn):
        i = row_of(turn)
        return pltpu.make_async_copy(
            field.at[pl.ds(0, nj), i], cells.at[0, i + 1, pl.ds(1, nj), inner],
            load_sem.at[jnp.minimum(turn, 2)],
        )

    def load_edge(side):
        i = row_of(0)
        return pltpu.make_async_copy(
            field.at[pl.ds(0, nj), i, 0 if side == 0 else nk - 1],
            cells.at[0, i + 1, pl.ds(1, nj), edge(side)], load_sem.at[3 * side])

    def load_between():
        i = row_of(0)
        return pltpu.make_async_copy(
            field.at[pl.ds(0, nj), i, pl.ds(1, nk - 2)],
            cells.at[0, i + 1, pl.ds(1, nj), pl.ds(LEVEL + 1, nk - 2)], load_sem.at[0])

    def loaded(first, count):
        start = jnp.where(upward, first, ni - first - count)
        part = cells.at[0, pl.ds(start + 1, count), pl.ds(1, nj), inner]
        pltpu.make_async_copy(part, part, load_sem.at[first]).wait()

    def load_flows(turn):
        i = row_of(turn)
        for d, source in enumerate((flow_j, flow_i, flow_k)):
            pltpu.make_async_copy(
                source.at[pl.ds(0, nj), i], flows.at[d, i], flow_sem.at[jnp.where(turn < 2, 0, 1)]
            ).start()

    def flows_loaded(group):
        rows = rows_of(0, 2) if group == 0 else rows_of(2, early)
        part = flows.at[pl.ds(0, 3), rows]
        pltpu.make_async_copy(part, part, flow_sem.at[group]).wait()

    def edge(side):
        return LEVEL if side == 0 else LEVEL + nk - 1

    def halo(side):
        return LEVEL - 1 if side == 0 else LEVEL + nk

    def k_copy(slot, side, i):
        part = pl.ds(1, nj)
        return pltpu.make_async_remote_copy(
            cells.at[slot, i + 1, part, edge(side)], cells.at[slot, i + 1, part, halo(1 - side)],
            k_send.at[slot], k_recv.at[slot, i],
            device_id=beside("down", side), device_id_type=MESH,
        )

    def half_span(part):
        return pl.ds(1 + part * (nj // 2), nj // 2)

    def half_recv(slot, i, part):
        return k_recv.at[slot, i] if part == 0 else k_last

    def k_half(slot, side, i, part):
        return pltpu.make_async_remote_copy(
            cells.at[slot, i + 1, half_span(part), edge(side)],
            cells.at[slot, i + 1, half_span(part), halo(1 - side)],
            k_send.at[slot], half_recv(slot, i, part),
            device_id=beside("down", side), device_id_type=MESH,
        )

    def k_all(slot, rows, span, neighbours, arrival):
        part = cells.at[slot, rows, span, pl.ds(LEVEL, neighbours)]
        return pltpu.make_async_remote_copy(
            part, part, k_send.at[slot], arrival,
            device_id=beside("down", 0), device_id_type=MESH,
        )

    def i_copy(slot, side):
        part = pl.ds(1, nj)
        return pltpu.make_async_remote_copy(
            cells.at[slot, 1 if side == 0 else ni, part, inner],
            cells.at[slot, ni + 1 if side == 0 else 0, part, inner],
            i_send.at[side], i_recv.at[slot, 1 - side],
            device_id=beside("east", side), device_id_type=MESH,
        )

    def j_copy(slot, side, group):
        rows = pl.ds(jnp.where(upward, group * half, ni - (group + 1) * half) + 1, half)
        sending, receiving = (side, 1 - side) if n_south > 2 else (0, 0)
        return pltpu.make_async_remote_copy(
            cells.at[slot, rows, 1 if side == 0 else nj, inner],
            cells.at[slot, rows, nj + 1 if side == 0 else 0, inner],
            j_send.at[sending, group], j_recv.at[slot, receiving, group],
            device_id=beside("south", side), device_id_type=MESH,
        )

    def edge_turn(side):
        return jnp.where(upward == (side == 0), 0, ni - 1)

    def each_k(act):
        if n_down > 1:
            inside = has("down", 0) & has("down", 1)
            pl.when(inside)(lambda: act(2))
            pl.when(jnp.logical_not(inside))(lambda: act(1))

    def sent(slot):
        each_k(lambda count: k_all(
            slot, pl.ds(1, ni), pl.ds(1, nj), count, k_recv.at[slot, 0]).wait_send())

    def half_received(slot, turn, part):
        i = row_of(turn)
        each_k(lambda count: k_all(
            slot, pl.ds(i + 1, 1), half_span(part), count, half_recv(slot, i, part)).wait_recv())

    def received(slot, turn):
        i = row_of(turn)
        each_k(lambda count: k_all(
            slot, pl.ds(i + 1, 1), pl.ds(1, nj), count, k_recv.at[slot, i]).wait_recv())
        sides_received(slot, turn)

    def sides_received(slot, turn):
        for side in (0, 1):
            pl.when(has("east", side) & (turn == edge_turn(side)))(
                lambda: i_copy(slot, 1 - side).wait_recv())
        for group in (0, 1):
            for side in (0, 1):
                pl.when(has("south", side) & (turn == group * half))(
                    lambda: j_copy(slot, 1 - side, group).wait_recv())

    def send_k(slot, side, turn):
        pl.when(has("down", side))(lambda: k_copy(slot, side, row_of(turn)).start())

    def send(slot, turn, final):
        ending = final & (turn == ni - 1)

        @pl.when(jnp.logical_not(ending | (final & upward)))
        def _():
            for side in (0, 1):
                send_k(slot, side, turn)

        @pl.when(ending)
        def _():
            @pl.when(upward)
            def _():
                @pl.loop(0, ni - 1)
                def _(other):
                    for side in (0, 1):
                        send_k(slot, side, other)

            i = row_of(turn)
            for part in (0, 1):
                for side in (0, 1):
                    pl.when(has("down", side))(lambda: k_half(slot, side, i, part).start())


        for side in (0, 1):
            @pl.when(has("east", side) & (turn == edge_turn(side)))
            def _():
                i_copy(slot, side).wait_send()
                i_copy(slot, side).start()
        for group in (0, 1):
            for side in (0, 1):
                @pl.when(has("south", side) & (turn == (group + 1) * half - 1))
                def _():
                    j_copy(slot, side, group).wait_send()
                    j_copy(slot, side, group).start()

    zero = jnp.zeros((nk, levels), jnp.float32)

    for side in (0, 1):
        load_edge(side).start()

    barrier = pltpu.get_barrier_semaphore()
    lower = south
    for offset in range(1, n_south):
        @pl.when(south + offset < n_south)
        def _():
            pl.semaphore_signal(barrier, 1, device_id={"south": south + offset},
                                device_id_type=MESH)
    lower = lower + has("down", 0).astype(jnp.int32)

    @pl.when(has("down", 1))
    def _():
        pl.semaphore_signal(barrier, 1, device_id=beside("down", 1), device_id_type=MESH)

    easts = jnp.int32(0)
    for side in (0, 1):
        easts = easts + has("east", side).astype(jnp.int32)

        @pl.when(upward & has("east", side))
        def _():
            pl.semaphore_signal(barrier, 1, device_id=beside("east", side), device_id_type=MESH)
    lower = lower + jnp.where(upward, 0, easts)

    @pl.loop(1, ni)
    def _(turn):
        load(turn).start()

    pl.when(lower > 0)(lambda: pl.semaphore_wait(barrier, lower))

    @pl.when(has("down", 0))
    def _():
        pl.semaphore_signal(ready_down, 1, device_id=beside("down", 0), device_id_type=MESH)

    for side in (0, 1):
        @pl.when(jnp.logical_not(upward) & has("east", side))
        def _():
            pl.semaphore_signal(ready_east, 1, device_id=beside("east", side),
                                device_id_type=MESH)
    for offset in range(1, n_south):
        @pl.when(south - offset >= 0)
        def _():
            pl.semaphore_signal(ready_south, 1, device_id={"south": south - offset},
                                device_id_type=MESH)

    load_edge(0).wait()
    send_k(0, 0, 0)
    load_between().start()
    load_edge(1).wait()
    loaded(1, 1)
    send_k(0, 0, 1)
    pl.when(has("down", 1))(lambda: pl.semaphore_wait(ready_down, 1))
    for turn in (0, 1):
        send_k(0, 1, turn)
    loaded(2, early)
    load_between().wait()

    @pl.loop(2, ni)
    def _(turn):
        for side in (0, 1):
            send_k(0, side, turn)

    @pl.loop(0, ni)
    def _(turn):
        load_flows(turn)

    pl.when(upward & (easts > 0))(lambda: pl.semaphore_wait(ready_east, easts))
    for side in (0, 1):
        pl.when(has("east", side))(lambda: i_copy(0, side).start())
    if n_south > 1:
        pl.when(has("south", 1))(lambda: pl.semaphore_wait(ready_south, n_south - 1 - south))
    for group in (0, 1):
        for side in (0, 1):
            pl.when(has("south", side))(lambda: j_copy(0, side, group).start())

    for side in (0, 1):
        @pl.when(jnp.logical_not(has("down", side)))
        def _():
            @pl.loop(0, ni)
            def _(i):
                @pl.loop(0, blocks)
                def _(block):
                    for slot in (0, 1):
                        cells[slot, i + 1, pl.ds(block * BLOCK + 1, BLOCK), halo(side)] = (
                            jnp.zeros((BLOCK, levels), jnp.float32))

        @pl.when(jnp.logical_not(has("east", side)))
        def _():
            @pl.loop(0, nj)
            def _(j):
                for slot in (0, 1):
                    cells[slot, 0 if side == 0 else ni + 1, j + 1, inner] = zero

        @pl.when(jnp.logical_not(has("south", side)))
        def _():
            @pl.loop(0, ni)
            def _(i):
                for slot in (0, 1):
                    cells[slot, i + 1, 0 if side == 0 else nj + 1, inner] = zero

    def advanced(slot, i, j):
        here = pl.ds(j + 1, BLOCK)
        column = cells[slot, i + 1, pl.ds(j, BLOCK + 2), inner]
        middle = column[1:BLOCK + 1]
        sides = (
            (column[:BLOCK], column[2:]),
            (cells[slot, i, here, inner], cells[slot, i + 2, here, inner]),
            (cells[slot, i + 1, here, pl.ds(LEVEL - 1, nk)],
             cells[slot, i + 1, here, pl.ds(LEVEL + 1, nk)]),
        )
        above, moved = None, None
        for d, (low, high) in enumerate(sides):
            share = flows[d, i, pl.ds(j, BLOCK)] * (low - high)
            above = high if d == 0 else above + high
            moved = share if d == 0 else moved + share
        return (0.7 * middle + 0.1 * above) + moved

    def raise_flows(i):
        @pl.loop(0, blocks)
        def _(block):
            here = pl.ds(pl.multiple_of(block * BLOCK, BLOCK), BLOCK)
            for d in range(3):
                flows[d, i, here] = flows[d, i, here] + 0.05

    @pl.loop(1, steps)
    def _(step):
        now, later = lax.rem(step + 1, 2), lax.rem(step, 2)

        @pl.loop(0, ni)
        def _(turn):
            i = row_of(turn)
            for group, first in enumerate((0, 2)):
                pl.when((step == 1) & (turn == first))(lambda: flows_loaded(group))
            pl.when(step == 1)(lambda: raise_flows(i))
            pl.when((step >= 2) & (turn == 0))(lambda: sent(later))
            received(now, turn)

            @pl.loop(0, blocks, unroll=2)
            def _(block):
                j = pl.multiple_of(block * BLOCK, BLOCK)
                values = advanced(now, i, j)
                cells[later, i + 1, pl.ds(j + 1, BLOCK), inner] = values

            send(later, turn, step == steps - 1)

    now = (steps - 1) % 2

    def stat_copy(offset, owner, part):
        target = lax.rem(south + offset, n_south)
        rows = rows_of(0, early) if part == 0 else rows_of(early, 2)
        return pltpu.make_async_remote_copy(
            stats.at[owner, rows], stats.at[owner, rows],
            stat_send.at[offset - 1], stat_recv.at[offset - 1, part],
            device_id={"south": target}, device_id_type=MESH,
        )

    def finish(turn, waits):
        i = row_of(turn)

        def store(j):
            values = advanced(now, i, j)
            end[pl.ds(j, BLOCK), i] = values
            return values

        def block(b, sums):
            away = store(pl.multiple_of(b * BLOCK, BLOCK)) - shift
            return sums[0] + jnp.sum(away, axis=0), sums[1] + jnp.sum(away * away, axis=0)

        count = blocks // len(waits)
        for part, wait in enumerate(waits):
            wait()
            first = part * count
            if part == 0:
                start = [store(b * BLOCK) for b in range(4)]
                shift = jnp.sum(sum(start), axis=0) * (1.0 / (len(start) * BLOCK))
                away = [values - shift for values in start]
                sums = (jnp.sum(sum(away), axis=0), jnp.sum(sum(a * a for a in away), axis=0))
                first = len(start)
            sums = lax.fori_loop(first, (part + 1) * count, block, sums, unroll=4)
        stats[south, i, 0] = shift + sums[0] * (1.0 / nj)
        stats[south, i, 1] = jnp.maximum(sums[1] - sums[0] * sums[0] * (1.0 / nj), 0.0)

    def send_stats(part):
        for offset in range(1, n_south):
            stat_copy(offset, south, part).start()

    @pl.loop(0, ni - 1)
    def _(turn):
        finish(turn, [lambda: received(now, turn)])
        pl.when(turn == early - 1)(lambda: send_stats(0))

    sides_received(now, ni - 1)
    finish(ni - 1, [lambda: half_received(now, ni - 1, 0), lambda: half_received(now, ni - 1, 1)])
    send_stats(1)

    for slot in (0, 1):
        sent(slot)
    for side in (0, 1):
        pl.when(has("east", side))(lambda: i_copy(now, side).wait_send())
        for group in (0, 1):
            pl.when(has("south", side))(lambda: j_copy(now, side, group).wait_send())

    for part, (first, count) in enumerate(((0, early), (early, 2))):
        for offset in range(1, n_south):
            owner = lax.rem(south + n_south - offset, n_south)
            stat_copy(offset, owner, part).wait_recv()

        @pl.loop(first, first + count)
        def _(turn):
            i = row_of(turn)
            whole_mean = stats[0, i, 0]
            for other in range(1, n_south):
                whole_mean = whole_mean + stats[other, i, 0]
            whole_mean = whole_mean * (1.0 / n_south)
            whole_squares = zero
            for other in range(n_south):
                away = stats[other, i, 0] - whole_mean
                whole_squares = whole_squares + (stats[other, i, 1] + nj * (away * away))
            mean_out[i] = whole_mean
            scale_out[i] = lax.rsqrt(whole_squares * (1.0 / (nj * n_south)) + 0.0001)

    for offset in range(1, n_south):
        whole = stats.at[south]
        pltpu.make_async_copy(whole, whole, stat_send.at[offset - 1]).wait()


def scale(pieces, values, mean, factor, standardized, copied, scaled, copy_sem, scale_sem):
    rows = values.shape[0] // pieces

    def copy_out(c):
        part = pl.ds(c * rows, rows)
        return pltpu.make_async_copy(values.at[part], copied.at[part], copy_sem)

    def scale_out(c):
        part = pl.ds(c * rows, rows)
        return pltpu.make_async_copy(scaled.at[part], standardized.at[part], scale_sem)

    @pl.loop(0, pieces)
    def _(c):
        copy_out(c).start()

    @pl.loop(0, pieces)
    def _(c):
        @pl.loop(0, rows)
        def _(offset):
            r = c * rows + offset
            scaled[r] = (values[r] - mean[...]) * factor[...]

        scale_out(c).start()

    pltpu.make_async_copy(values, copied, copy_sem).wait()
    pltpu.make_async_copy(scaled, standardized, scale_sem).wait()


def per_device(counts, field_values, flow_j, flow_i, flow_k):
    nj, ni, nk, levels = field_values.shape
    n_south = counts[0]
    plane = (ni, nk, levels)
    whole = jax.ShapeDtypeStruct(field_values.shape, jnp.float32)
    vmem = pl.BlockSpec(memory_space=pltpu.VMEM)
    hbm = pl.BlockSpec(memory_space=pltpu.HBM)
    dma = pltpu.SemaphoreType.DMA
    regular = pltpu.SemaphoreType.REGULAR
    others = max(n_south - 1, 1)
    sides = 2 if n_south > 2 else 1
    end, mean, factor = pl.pallas_call(
        functools.partial(transport, counts, STEPS),
        name="transport",
        out_shape=(
            whole,
            jax.ShapeDtypeStruct(plane, jnp.float32),
            jax.ShapeDtypeStruct(plane, jnp.float32),
        ),
        in_specs=[hbm] * 4,
        out_specs=(vmem,) * 3,
        scratch_shapes=[
            pltpu.VMEM((2, ni + 2, nj + 2, nk + 2 * LEVEL, levels), jnp.float32),
            pltpu.VMEM((3, ni, nj, nk, levels), jnp.float32),
            pltpu.VMEM((n_south, ni, 2, nk, levels), jnp.float32),
            regular,
            regular,
            regular,
            dma((4,)),
            dma((2,)),
            dma((2,)),
            dma((2, ni)),
            dma,
            dma((2,)),
            dma((2, 2)),
            dma((sides, 2)),
            dma((2, sides, 2)),
            dma((others,)),
            dma((others, 2)),
        ],
        compiler_params=pltpu.CompilerParams(
            collective_id=0, has_side_effects=True, vmem_limit_bytes=46 * 2**20
        ),
    )(*(pltpu.with_memory_space_constraint(array, pltpu.HBM)
        for array in (field_values, flow_j, flow_i, flow_k)))
    pieces = 4
    return pl.pallas_call(
        functools.partial(scale, pieces),
        name="scale",
        in_specs=[vmem] * 3,
        out_specs=(hbm, hbm),
        out_shape=(whole, whole),
        scratch_shapes=[
            pltpu.VMEM(field_values.shape, jnp.float32),
            dma,
            dma,
        ],
        compiler_params=pltpu.CompilerParams(vmem_limit_bytes=16 * 2**20),
    )(end, mean, factor)


def solution(mesh):
    counts = tuple(mesh.shape[axis] for axis in ("south", "east", "down"))
    spec = P("south", "east", "down", None)
    return jax.shard_map(
        functools.partial(per_device, counts),
        mesh=mesh,
        in_specs=(spec,) * 4,
        out_specs=(spec, spec),
        check_vma=False,
    )
```
